256 devices in a mesh: sample: 16 (over z, y_hi), span: 8 (over x, y_lo), kvhead: 2 (over core).
Axes of the slice: x: 4, y: 4 (y_hi: 2, y_lo: 2; y = y_hi * 2 + y_lo), z: 8, core: 2. Of those that a mesh axis runs over, the one named last changes fastest.
Arguments:
- queries: bfloat16 [16, 256, 3584], P('sample', None, 'kvhead'), may hold values from -6 to 6
- outputs: bfloat16 [16, 256, 3584], P('sample', None, 'kvhead'), may hold values from -6 to 6
- grad_out: bfloat16 [16, 256, 3584], P('sample', None, 'kvhead'), may hold values from -48 to 48
- log_norms: float32 [16, 28, 256], P('sample', 'kvhead'), as said below
- lengths: int32 [16], P('sample'), may hold values from 1 to 256, 1024 in all
- prompt_key_rows: bfloat16 [16384, 512], P(('sample', 'span'), 'kvhead'), may hold values from -9 to 9
- prompt_value_rows: bfloat16 [16384, 512], P(('sample', 'span'), 'kvhead'), may hold values from -6 to 6
- slice_key_rows: bfloat16 [16, 256, 512], P('sample', 'span', 'kvhead'), may hold values from -9 to 9
- slice_value_rows: bfloat16 [16, 256, 512], P('sample', 'span', 'kvhead'), may hold values from -6 to 6
Outputs:
- grad_queries: bfloat16 [16, 256, 3584], P('sample', 'span', 'kvhead')
- grad_k_prompt: bfloat16 [16384, 512], P(('sample', 'span'), 'kvhead')
- grad_v_prompt: bfloat16 [16384, 512], P(('sample', 'span'), 'kvhead')
- grad_k_self: bfloat16 [16, 256, 512], P('sample', 'span', 'kvhead')
- grad_v_self: bfloat16 [16, 256, 512], P('sample', 'span', 'kvhead')
The draws below stay inside these ranges and needn't reach their ends.
Inputs may be any that keep to these rules, and one draw needn't show every extreme that they name: `log_norms`: every entry lies between 0.8 and 2.4 above the natural logarithm of 16640.
All inputs are finite; a program needn't handle non-finite values. No bound on the sum of `lengths` on one device may be relied on, other than what follows from the above.
Results may differ from the reference program's by a relative error of at most 0.0051.
Values may be sent and summed in bfloat16 or wider, within the bound.
No kernel may reach another device: no remote copies, remote signals or barrier semaphores. Data moves between devices by JAX's collectives and lax.ppermute only.
A program may use at most 64 MiB of HBM per device.

```python
import math
import jax
import jax.numpy as jnp
import numpy as np
from jax import lax

QUERY_HEADS = 28
KEY_VALUE_HEADS = 4
HEAD_WIDTH = 128
SLICE_LENGTH = 256
SAMPLE_COUNT = 16
PROMPT_LENGTH = 16384


def draw_log_norms(key, part):
    base_level = math.log(PROMPT_LENGTH + SLICE_LENGTH) + 1.1
    offsets = jax.random.uniform(key, (SAMPLE_COUNT, QUERY_HEADS, SLICE_LENGTH), jnp.float32, 0.0, 1.0)
    return (base_level + offsets).astype(jnp.float32)


def block_scale(own_key, extent, pieces, smallest, largest):
    gain, own = 1.0, jax.random.fold_in(own_key, 6)
    for dim, shards_of in pieces:
        steps = jnp.exp(jax.random.uniform(jax.random.fold_in(own, dim), (shards_of,), jnp.float32, smallest / len(pieces), largest / len(pieces)))
        gain = gain * jnp.repeat(steps, extent[dim] // shards_of).reshape([-1 if axis == dim else 1 for axis in range(len(extent))])
    return gain


def length_profile(number_of, total, reach, slope):
    loads = [(1 << 20) // math.isqrt(grade ** slope) + 1 for grade in range(2, number_of + 1)]
    spare, given = total - reach - (number_of - 1), [1] * (number_of - 1)
    while spare > 0:
        free = [i for i in range(number_of - 1) if given[i] < reach]
        mass, budget = sum([loads[i] for i in free]), spare
        for i in free:
            addition = min(reach - given[i], max(1, budget * loads[i] // mass), spare)
            given[i] = given[i] + addition
            spare = spare - addition
    return np.array([reach] + given)


def uneven(own_key, count, total, limit, skew):
    if count == 2:
        one = jax.random.randint(own_key, (), max(1, total - limit), min(limit, total - 1) + 1)
        return jnp.stack([one, total - one])
    sizes = jnp.asarray(length_profile(count, total, limit, skew), jnp.int32)
    twos = (count - 1) // 2
    source_of, taker = sizes[1:1 + 2 * twos:2], sizes[2:2 + 2 * twos:2]
    slack = jnp.minimum(source_of - 1, limit - taker)
    passed = jax.random.randint(jax.random.fold_in(own_key, 1), (twos,), 0, 1 << 20) % (slack + 1)
    sizes = sizes.at[1:1 + 2 * twos:2].set(source_of - passed).at[2:2 + 2 * twos:2].set(taker + passed)
    return sizes[jax.random.permutation(jax.random.fold_in(own_key, 2), count)]


def centred(key, extent, spread, limit, split=(), dtype=jnp.bfloat16):
    loudness = block_scale(key, extent, split, -0.22, 0.18) if split else 1.0
    values = jax.random.normal(key, extent, jnp.float32) * spread * loudness
    return jnp.minimum(jnp.maximum(values, -limit), limit).astype(dtype)


def setup_inputs(seed: int = 0) -> dict:
    key_of = jax.random.split(jax.random.key(seed), 10)
    queries = centred(key_of[0], (SAMPLE_COUNT, SLICE_LENGTH, QUERY_HEADS * HEAD_WIDTH), 1.0, 6.0, ((0, 16), (2, 2)))
    outputs = centred(key_of[1], (SAMPLE_COUNT, SLICE_LENGTH, QUERY_HEADS * HEAD_WIDTH), 1.0, 6.0, ((0, 16), (2, 2)))
    grad_out = centred(key_of[2], (SAMPLE_COUNT, SLICE_LENGTH, QUERY_HEADS * HEAD_WIDTH), 8.0, 48.0, ((0, 16), (2, 2)))
    log_norms = draw_log_norms(jax.random.fold_in(key_of[9], 71), 0)
    lengths = uneven(key_of[4], SAMPLE_COUNT, SAMPLE_COUNT * SLICE_LENGTH // 4, SLICE_LENGTH, 2).astype(jnp.int32)
    prompt_key_rows = centred(key_of[5], (PROMPT_LENGTH, KEY_VALUE_HEADS * HEAD_WIDTH), 1.5, 9.0, ((0, 128), (1, 2)))
    prompt_value_rows = centred(key_of[6], (PROMPT_LENGTH, KEY_VALUE_HEADS * HEAD_WIDTH), 1.0, 6.0, ((0, 128), (1, 2)))
    slice_key_rows = centred(key_of[7], (SAMPLE_COUNT, SLICE_LENGTH, KEY_VALUE_HEADS * HEAD_WIDTH), 1.5, 9.0, ((0, 16), (1, 8), (2, 2)))
    slice_value_rows = centred(key_of[8], (SAMPLE_COUNT, SLICE_LENGTH, KEY_VALUE_HEADS * HEAD_WIDTH), 1.0, 6.0, ((0, 16), (1, 8), (2, 2)))
    return {"queries": queries, "outputs": outputs, "grad_out": grad_out, "log_norms": log_norms, "lengths": lengths, "prompt_key_rows": prompt_key_rows, "prompt_value_rows": prompt_value_rows, "slice_key_rows": slice_key_rows, "slice_value_rows": slice_value_rows}


def divide_heads(matrix, head_count):
    return matrix.reshape(matrix.shape[0], head_count, HEAD_WIDTH).transpose(1, 0, 2)

def join_heads(blocks):
    return blocks.transpose(1, 0, 2).reshape(blocks.shape[1], blocks.shape[0] * HEAD_WIDTH)

def reference(queries, outputs, grad_out, log_norms, lengths, prompt_key_rows, prompt_value_rows, slice_key_rows, slice_value_rows):
    query_group_width = QUERY_HEADS // KEY_VALUE_HEADS
    score_scale = 1.0 / math.sqrt(HEAD_WIDTH)
    expanded_key_heads = divide_heads(prompt_key_rows, KEY_VALUE_HEADS)
    expanded_value_heads = divide_heads(prompt_value_rows, KEY_VALUE_HEADS)
    row_pos = lax.broadcasted_iota(jnp.int32, (query_group_width * SLICE_LENGTH,), 0) % SLICE_LENGTH
    col_pos = lax.broadcasted_iota(jnp.int32, (SLICE_LENGTH,), 0)
    visible_mask = col_pos[None, :] <= row_pos[:, None]

    def to_groups(input_array):
        return input_array.reshape(SLICE_LENGTH, KEY_VALUE_HEADS, query_group_width, HEAD_WIDTH).transpose(1, 2, 0, 3).reshape(KEY_VALUE_HEADS, query_group_width * SLICE_LENGTH, HEAD_WIDTH)

    def one_sample(carry, inputs):
        query, output, grad, saved_log_norms, length, slice_key_head, slice_value_head = inputs
        q_rows = to_groups(query)
        o_rows = to_groups(output)
        live_rows = row_pos < length
        g_rows = jnp.where(live_rows[None, :, None], to_groups(grad), jnp.zeros((), jnp.bfloat16))
        per_row_norms = saved_log_norms.reshape(KEY_VALUE_HEADS, query_group_width * SLICE_LENGTH)
        slice_keys = divide_heads(slice_key_head, KEY_VALUE_HEADS)
        slice_values = divide_heads(slice_value_head, KEY_VALUE_HEADS)

        def one_head(call_arguments):
            query_head, output_head, output_grad_head, head_log_norm, prompt_key_head, prompt_value_head, slice_key_single, slice_value_single = call_arguments
            row_delta = lax.optimization_barrier(jnp.sum(output_grad_head.astype(jnp.float32) * output_head.astype(jnp.float32), axis=-1))

            def partial_terms(keys, values, mask):
                scores = jnp.dot(query_head, keys.T, preferred_element_type=jnp.float32) * score_scale
                prob_rows = jnp.exp(scores - head_log_norm[:, None])
                if mask is not None:
                    prob_rows = jnp.where(mask, prob_rows, 0.0)
                dprobs = jnp.dot(output_grad_head, values.T, preferred_element_type=jnp.float32)
                score_grads = (prob_rows * (dprobs - row_delta[:, None])).astype(jnp.bfloat16)
                prob_low = prob_rows.astype(jnp.bfloat16)
                query_grad = jnp.dot(score_grads, keys, preferred_element_type=jnp.float32) * score_scale
                key_grad = jnp.dot(score_grads.T, query_head, preferred_element_type=jnp.float32) * score_scale
                value_grad = jnp.dot(prob_low.T, output_grad_head, preferred_element_type=jnp.float32)
                return (query_grad, key_grad, value_grad)
            query_prompt, key_prompt, value_prompt = partial_terms(prompt_key_head, prompt_value_head, None)
            slice_query_rows, slice_key_gradient, slice_value_gradient = partial_terms(slice_key_single, slice_value_single, visible_mask)
            return (query_prompt + slice_query_rows, key_prompt, value_prompt, slice_key_gradient, slice_value_gradient)
        query_rows_every, key_prompt, value_prompt, slice_key_gradient, slice_value_gradient = lax.map(one_head, (q_rows, o_rows, g_rows, per_row_norms, expanded_key_heads, expanded_value_heads, slice_keys, slice_values))
        flattened_query = query_rows_every.reshape(KEY_VALUE_HEADS, query_group_width, SLICE_LENGTH, HEAD_WIDTH).transpose(2, 0, 1, 3).reshape(SLICE_LENGTH, QUERY_HEADS * HEAD_WIDTH)
        new_carry = (carry[0] + join_heads(key_prompt), carry[1] + join_heads(value_prompt))
        return (new_carry, (flattened_query.astype(jnp.bfloat16), join_heads(slice_key_gradient).astype(jnp.bfloat16), join_heads(slice_value_gradient).astype(jnp.bfloat16)))
    starting_state = (jnp.zeros((PROMPT_LENGTH, KEY_VALUE_HEADS * HEAD_WIDTH), jnp.float32), jnp.zeros((PROMPT_LENGTH, KEY_VALUE_HEADS * HEAD_WIDTH), jnp.float32))
    sums, stacked = lax.scan(one_sample, starting_state, (queries, outputs, grad_out, log_norms, lengths, slice_key_rows, slice_value_rows))
    return (stacked[0], sums[0].astype(jnp.bfloat16), sums[1].astype(jnp.bfloat16), stacked[1], stacked[2])
```

```python
import math

import jax
import jax.numpy as jnp
from jax import lax
from jax.experimental import pallas as pl
from jax.experimental.pallas import tpu as pltpu
from jax.sharding import Mesh
from jax.sharding import PartitionSpec as P

HEAD_WIDTH = 128
SAMPLE = ("sample_0", "sample_1")
PLANE = ("sample_1", "span")
SAMPLE_SPAN = ("sample_0", "sample_1", "span")
GROUP = 7
CLASSES = 8
SLOTS = 18
INTERPRET = False
BF16 = jnp.bfloat16
F32 = jnp.float32
SCALE = 1.0 / math.sqrt(HEAD_WIDTH)


def exchange(tiles, axes):
    return lax.all_to_all(tiles, axes, split_axis=0, concat_axis=0, tiled=True)


def dot(a, b, ca, cb):
    return lax.dot_general(a, b, (((ca,), (cb,)), ((), ())), preferred_element_type=F32)


def call(body, out_shape, *args, **kw):
    return pl.pallas_call(body, out_shape=out_shape, interpret=INTERPRET, **kw)(*args)


def pick_kernel(info, q_ref, g_ref, out_ref):
    p, off, live = info[0], info[1], info[2]
    shape = (64, 512)
    row = lax.broadcasted_iota(jnp.int32, shape, 0)
    col = lax.broadcasted_iota(jnp.int32, shape, 1)
    i = col % 256
    hit = (
        (i % CLASSES == p)
        & (i < live)
        & ((off + i // CLASSES) % 8 == row // 8)
        & (i // 64 == row % 4)
        & (col // 256 == (row // 4) % 2)
    )
    pick = jnp.where(hit, 1.0, 0.0).astype(BF16)
    for head in range(2 * GROUP):
        lanes = slice(head * HEAD_WIDTH, (head + 1) * HEAD_WIDTH)
        both = jnp.concatenate([q_ref[:, lanes], g_ref[:, lanes]], axis=0)
        rows = dot(pick, both, 1, 0).astype(BF16)
        out_ref[:, head // GROUP, head % GROUP] = rows.reshape(8, 8, HEAD_WIDTH)


def place_kernel(dest_ref, rows_ref, out_ref):
    total = out_ref.shape[0]
    dest = dest_ref[0:1, :]
    hit = lax.broadcasted_iota(jnp.int32, (total, dest.shape[1]), 0) == dest
    out_ref[...] = dot(jnp.where(hit, 1.0, 0.0).astype(BF16), rows_ref[...], 1, 0).astype(BF16)


def place(dest, rows, total):
    return call(
        place_kernel, jax.ShapeDtypeStruct((total, HEAD_WIDTH), BF16), dest[None, :], rows
    )


def sum_place_kernel(dest_ref, parts_ref, out_ref):
    total = out_ref.shape[0]
    rows = parts_ref[0].astype(F32)
    for k in range(1, parts_ref.shape[0]):
        rows = rows + parts_ref[k].astype(F32)
    hit = lax.broadcasted_iota(jnp.int32, (rows.shape[0], total), 0) == dest_ref[0:1, :]
    pick = jnp.where(hit, 1.0, 0.0).astype(BF16)
    out_ref[...] = dot(pick, rows.astype(BF16), 0, 0).astype(BF16)


def prompt_kernel(kv_ref, rows_ref, norm_ref, kvg_ref, gq_ref, acc_ref):
    step = pl.program_id(0)

    @pl.when(step == 0)
    def _():
        acc_ref[...] = jnp.zeros_like(acc_ref)

    keys = kv_ref[:, 0:128, :].reshape(-1, HEAD_WIDTH)
    values = kv_ref[:, 128:256, :].reshape(-1, HEAD_WIDTH)
    gk = jnp.zeros(keys.shape, F32)
    gv = jnp.zeros(keys.shape, F32)
    for part in range(4):
        q = rows_ref[2 * part : 2 * part + 2, 0:128, :].reshape(256, HEAD_WIDTH)
        g = rows_ref[2 * part : 2 * part + 2, 128:256, :].reshape(256, HEAD_WIDTH)
        lanes = slice(256 * part, 256 * part + 256)
        prob = jnp.exp(dot(keys, q, 1, 1) * SCALE - norm_ref[0:1, lanes])
        sgrad = (prob * (dot(values, g, 1, 1) - norm_ref[1:2, lanes])).astype(BF16)
        gv = gv + dot(prob.astype(BF16), g, 1, 0)
        gk = gk + dot(sgrad, q, 1, 0)
        acc_ref[lanes, :] += dot(sgrad, keys, 0, 0)
    kvg_ref[:, 0:128, :] = (gk * SCALE).astype(BF16).reshape(-1, 128, HEAD_WIDTH)
    kvg_ref[:, 128:256, :] = gv.astype(BF16).reshape(-1, 128, HEAD_WIDTH)

    @pl.when(step == pl.num_programs(0) - 1)
    def _():
        gq_ref[...] = (acc_ref[...] * SCALE).astype(BF16)


def prompt_terms(kv, rows, norms):
    sources = kv.shape[0]
    per = 2
    block = pl.BlockSpec((per, 256, HEAD_WIDTH), lambda k: (k, 0, 0))
    return pl.pallas_call(
        prompt_kernel,
        grid=(sources // per,),
        in_specs=[
            block,
            pl.BlockSpec(rows.shape, lambda k: (0, 0, 0)),
            pl.BlockSpec(norms.shape, lambda k: (0, 0)),
        ],
        out_specs=[block, pl.BlockSpec((1024, HEAD_WIDTH), lambda k: (0, 0))],
        out_shape=[
            jax.ShapeDtypeStruct(kv.shape, BF16),
            jax.ShapeDtypeStruct((1024, HEAD_WIDTH), BF16),
        ],
        scratch_shapes=[pltpu.VMEM((1024, HEAD_WIDTH), F32)],
        interpret=INTERPRET,
    )(kv, rows, norms)


def key_sum_kernel(parts_ref, k_ref, v_ref):
    for head in range(2):
        total = parts_ref[head, 0].astype(F32)
        for k in range(1, parts_ref.shape[1]):
            total = total + parts_ref[head, k].astype(F32)
        lanes = slice(head * HEAD_WIDTH, (head + 1) * HEAD_WIDTH)
        k_ref[:, lanes] = total[0:128].astype(BF16)
        v_ref[:, lanes] = total[128:256].astype(BF16)


def self_kernel(
    info, q_ref, g_ref, norm_ref, delta_ref, col_norm_ref, col_delta_ref, own_ref, kv_ref,
    gk_ref, gv_ref, gq_ref,
):
    p, live = info[0], info[1]
    rows_total = q_ref.shape[0]
    i_row = lax.broadcasted_iota(jnp.int32, (32, rows_total), 1)
    j_row = lax.broadcasted_iota(jnp.int32, (32, rows_total), 0) + p * 32
    live_row = lax.broadcasted_iota(jnp.int32, (rows_total, HEAD_WIDTH), 0) < live
    live_own = lax.broadcasted_iota(jnp.int32, (32, HEAD_WIDTH), 0) + p * 32 < live
    zero = jnp.zeros((), BF16)
    for kv in range(2):
        key_lanes = slice(kv * HEAD_WIDTH, (kv + 1) * HEAD_WIDTH)
        value_lanes = slice((kv + 2) * HEAD_WIDTH, (kv + 3) * HEAD_WIDTH)
        keys, values = own_ref[:, key_lanes], own_ref[:, value_lanes]
        all_keys = kv_ref[:, :, key_lanes].reshape(rows_total, HEAD_WIDTH)
        all_values = kv_ref[:, :, value_lanes].reshape(rows_total, HEAD_WIDTH)
        gk = jnp.zeros((32, HEAD_WIDTH), F32)
        gv = jnp.zeros((32, HEAD_WIDTH), F32)
        for inner in range(GROUP):
            head = kv * GROUP + inner
            lanes = slice(head * HEAD_WIDTH, (head + 1) * HEAD_WIDTH)
            q = q_ref[:, lanes]
            g = jnp.where(live_row, g_ref[:, lanes], zero)
            prob = jnp.exp(dot(keys, q, 1, 1) * SCALE - norm_ref[head : head + 1, :])
            prob = jnp.where(j_row <= i_row, prob, 0.0)
            sgrad = prob * (dot(values, g, 1, 1) - delta_ref[head : head + 1, :])
            gv = gv + dot(prob.astype(BF16), g, 1, 0)
            gk = gk + dot(sgrad.astype(BF16), q, 1, 0)
            q_own = q_ref[pl.ds(pl.multiple_of(p * 32, 32), 32), lanes]
            g_own = g_ref[pl.ds(pl.multiple_of(p * 32, 32), 32), lanes]
            g_own = jnp.where(live_own, g_own, zero)
            prob = jnp.exp(dot(q_own, all_keys, 1, 1) * SCALE - col_norm_ref[:, head : head + 1])
            i_own = lax.broadcasted_iota(jnp.int32, prob.shape, 0) + p * 32
            prob = jnp.where(lax.broadcasted_iota(jnp.int32, prob.shape, 1) <= i_own, prob, 0.0)
            sgrad = prob * (dot(g_own, all_values, 1, 1) - col_delta_ref[:, head : head + 1])
            gq_ref[:, lanes] = dot(sgrad.astype(BF16), all_keys, 1, 0) * SCALE
        gk_ref[:, key_lanes] = (gk * SCALE).astype(BF16)
        gv_ref[:, key_lanes] = gv.astype(BF16)


def shards(
    queries,
    outputs,
    grad_out,
    log_norms,
    lengths,
    prompt_key_rows,
    prompt_value_rows,
    slice_key_rows,
    slice_value_rows,
):
    z = lax.axis_index("sample_0")
    half = lax.axis_index("sample_1")
    p = lax.axis_index("span")
    sample = 2 * z + half
    spans = lax.axis_size("span")
    slice_rows = queries.shape[1]
    heads = queries.shape[2] // HEAD_WIDTH
    q, o, g = queries[0], outputs[0], grad_out[0]
    norms = log_norms[0]
    live = lengths[0]

    kv_heads = jnp.concatenate(
        [
            prompt_key_rows.reshape(-1, 2, HEAD_WIDTH).transpose(1, 0, 2),
            prompt_value_rows.reshape(-1, 2, HEAD_WIDTH).transpose(1, 0, 2),
        ],
        axis=1,
    )
    kv_send = jnp.broadcast_to(kv_heads[:, None], (2, spans, *kv_heads.shape[1:]))
    kv = exchange(kv_send.reshape(2 * spans, *kv_heads.shape[1:]), PLANE)

    live_rows = lax.broadcasted_iota(jnp.int32, (slice_rows, 1), 0) < live
    g_live = jnp.where(live_rows, g, jnp.zeros((), BF16))
    delta = jnp.sum(
        (g_live.astype(F32) * o.astype(F32)).reshape(slice_rows, heads, HEAD_WIDTH), axis=-1
    ).T
    class_rows = slice_rows // CLASSES

    def of_class(x):
        return lax.dynamic_index_in_dim(x.reshape(heads, class_rows, CLASSES), p, 2, keepdims=False)

    stats = jnp.stack([of_class(norms), of_class(delta)])
    stats = stats.reshape(2, 2, GROUP * class_rows).transpose(1, 0, 2)
    stats = jnp.concatenate(
        [
            stats.reshape(2, 2 * GROUP * class_rows),
            jnp.broadcast_to(live.astype(F32), (2, 512 - 2 * GROUP * class_rows)),
        ],
        axis=1,
    )
    stats = exchange(jnp.broadcast_to(stats[None], (8, 2, 512)).reshape(16, 512), SAMPLE)
    all_lengths = stats[:, 2 * GROUP * class_rows].astype(jnp.int32)
    live_of = jnp.clip((all_lengths - p + CLASSES - 1) // CLASSES, 0, class_rows)
    before = lax.broadcasted_iota(jnp.int32, (16, 16), 1) < lax.broadcasted_iota(
        jnp.int32, (16, 16), 0
    )
    offset = jnp.sum(jnp.where(before, live_of[None, :], 0), axis=1)
    own_offset = jnp.sum(jnp.where(jnp.arange(16) == sample, offset, 0))

    picked = call(
        pick_kernel,
        jax.ShapeDtypeStruct((8, 2, GROUP, 8, HEAD_WIDTH), BF16),
        jnp.stack([p, own_offset, live]),
        q,
        g,
        in_specs=[
            pl.BlockSpec(memory_space=pltpu.SMEM),
            pl.BlockSpec(memory_space=pltpu.VMEM),
            pl.BlockSpec(memory_space=pltpu.VMEM),
        ],
    )
    arrived = exchange(picked.reshape(16, GROUP * 8, HEAD_WIDTH), SAMPLE)
    step4 = jnp.arange(4)[None, :]
    local = 8 * step4 + ((z - offset) % 8)[:, None]
    slot = jnp.where(local < live_of[:, None], (offset[:, None] + local) // 8, -4096)
    compact_dest = (
        slot[:, None, None, :]
        + SLOTS * jnp.arange(GROUP)[None, :, None, None]
        + 128 * jnp.arange(2)[None, None, :, None]
    )
    compact = place(compact_dest.reshape(-1), arrived.reshape(-1, HEAD_WIDTH), 256)
    rows = exchange(jnp.broadcast_to(compact[None], (8, 256, HEAD_WIDTH)), "sample_0")

    rank = 8 * jnp.arange(SLOTS)[None, :] + jnp.arange(8)[:, None]
    in_class = jnp.arange(class_rows)[None, :]
    rank_of = jnp.where(in_class < live_of[:, None], offset[:, None] + in_class, -1)
    chosen = (rank_of.reshape(-1)[:, None] == rank.reshape(-1)[None, :]).astype(F32)
    table = stats[:, : 2 * GROUP * class_rows].reshape(16, 2 * GROUP, class_rows)
    table = table.transpose(1, 0, 2).reshape(2 * GROUP, 16 * class_rows)
    row_stats = jnp.dot(table, chosen, precision=lax.Precision.HIGHEST)
    row_stats = row_stats.reshape(2, GROUP, 8, SLOTS).transpose(0, 2, 1, 3)
    row_stats = jnp.pad(
        row_stats.reshape(2, 8, GROUP * SLOTS), ((0, 0), (0, 0), (0, 128 - GROUP * SLOTS))
    ).reshape(2, 1024)

    own_kv = jnp.concatenate([slice_key_rows[0], slice_value_rows[0]], axis=1)
    slice_kv = exchange(jnp.broadcast_to(own_kv[None], (spans, *own_kv.shape)), "span")
    own_rows = slice_rows // spans
    col_norms = lax.dynamic_slice_in_dim(norms, p * own_rows, own_rows, 1).T
    col_delta = lax.dynamic_slice_in_dim(delta, p * own_rows, own_rows, 1).T
    own_shape = jax.ShapeDtypeStruct((own_rows, 2 * HEAD_WIDTH), BF16)
    gk_self, gv_self, gq_self = call(
        self_kernel,
        [own_shape, own_shape, jax.ShapeDtypeStruct((own_rows, heads * HEAD_WIDTH), F32)],
        jnp.stack([p, live]),
        q,
        g,
        norms,
        delta,
        col_norms,
        col_delta,
        own_kv,
        slice_kv,
        in_specs=[pl.BlockSpec(memory_space=pltpu.SMEM)]
        + [pl.BlockSpec(memory_space=pltpu.VMEM)] * 8,
    )

    kv_grads, gq_part = prompt_terms(kv, rows, row_stats)
    kv_parts = exchange(kv_grads, PLANE)
    prompt_shape = jax.ShapeDtypeStruct(prompt_key_rows.shape, BF16)
    gk_prompt, gv_prompt = call(
        key_sum_kernel,
        [prompt_shape, prompt_shape],
        kv_parts.reshape(2, spans, *kv_parts.shape[1:]),
    )

    gq_parts = exchange(gq_part.reshape(8, 128, HEAD_WIDTH), "sample_0")
    back = slot[:, None, :] + SLOTS * jnp.arange(8)[None, :, None]
    back = jnp.where(jnp.arange(8)[None, :, None] < GROUP, back, -1)
    returned = call(
        sum_place_kernel,
        jax.ShapeDtypeStruct((512, HEAD_WIDTH), BF16),
        back.reshape(1, 512),
        gq_parts,
    )
    returned = exchange(returned.reshape(16, 32, HEAD_WIDTH), SAMPLE)
    index = jnp.arange(512)
    from_z, from_head = index // 64, GROUP * ((index // 32) % 2) + (index % 32) // 4
    in_class = 8 * (index % 4) + (from_z - own_offset) % 8
    spread_dest = (in_class // 4) * (heads * 4) + from_head * 4 + in_class % 4
    spread_dest = jnp.where((index % 32) // 4 < GROUP, spread_dest, -1)
    spread = place(spread_dest, returned.reshape(512, HEAD_WIDTH), heads * slice_rows // CLASSES)
    final = exchange(spread.reshape(spans, heads * 4, HEAD_WIDTH), "span")
    gq_prompt = final.reshape(CLASSES, heads, 4, HEAD_WIDTH).transpose(2, 0, 1, 3)
    grad_query = (gq_prompt.reshape(own_rows, heads * HEAD_WIDTH).astype(F32) + gq_self).astype(BF16)
    return grad_query[None], gk_prompt, gv_prompt, gk_self[None], gv_self[None]


def solution(mesh):
    split = Mesh(
        mesh.devices.reshape(8, 2, mesh.shape["span"], mesh.shape["kvhead"]),
        ("sample_0", "sample_1", "span", "kvhead"),
    )
    placed = (
        P(SAMPLE, None, "kvhead"),
        P(SAMPLE, None, "kvhead"),
        P(SAMPLE, None, "kvhead"),
        P(SAMPLE, "kvhead", None),
        P(SAMPLE),
        P(SAMPLE_SPAN, "kvhead"),
        P(SAMPLE_SPAN, "kvhead"),
        P(SAMPLE, "span", "kvhead"),
        P(SAMPLE, "span", "kvhead"),
    )
    return jax.shard_map(
        shards,
        mesh=split,
        in_specs=placed,
        out_specs=(
            P(SAMPLE, "span", "kvhead"),
            P(SAMPLE_SPAN, "kvhead"),
            P(SAMPLE_SPAN, "kvhead"),
            P(SAMPLE, "span", "kvhead"),
            P(SAMPLE, "span", "kvhead"),
        ),
        check_vma=False,
    )
```

```python
import math

import jax
import jax.numpy as jnp
from jax import lax
from jax.experimental import pallas as pl
from jax.experimental.pallas import tpu as pltpu
from jax.sharding import Mesh
from jax.sharding import PartitionSpec as P

HEAD_WIDTH = 128
SAMPLE = ("sample_0", "sample_1")
PLANE = ("sample_1", "span")
SAMPLE_SPAN = ("sample_0", "sample_1", "span")
GROUP = 7
CLASSES = 8
SLOTS = 24
LIVE = 144
STATS = GROUP * HEAD_WIDTH
INTERPRET = False
BF16 = jnp.bfloat16
F32 = jnp.float32
SCALE = 1.0 / math.sqrt(HEAD_WIDTH)
EXACT = lax.Precision.HIGHEST


def exchange(tiles, axes):
    return lax.all_to_all(tiles, axes, split_axis=0, concat_axis=0, tiled=True)


def dot(a, b, ca, cb):
    return lax.dot_general(a, b, (((ca,), (cb,)), ((), ())), preferred_element_type=F32)


def call(body, out_shape, *args, **kw):
    return pl.pallas_call(body, out_shape=out_shape, interpret=INTERPRET, **kw)(*args)


def stat_lanes(shape):
    lane = lax.broadcasted_iota(jnp.int32, shape, 1)
    group = jnp.zeros(shape, jnp.int32)
    for edge in range(GROUP, 6 * GROUP, GROUP):
        group = group + jnp.where(lane >= edge, 1, 0)
    piece = jnp.where(group >= 3, group - 3, group)
    return lane, lane - GROUP * group, piece


def pick_kernel(info, q_ref, o_ref, g_ref, norm_ref, out_ref):
    p, turn, live = info[0], info[1], info[2]
    row = lax.broadcasted_iota(jnp.int32, (64, 256), 0)
    i = lax.broadcasted_iota(jnp.int32, (64, 256), 1)
    hit = (i % 8 == p) & (i < live) & ((turn + i // 8) % 8 == row // 8) & (i // 64 == row % 4)
    pick_q = jnp.where(hit & (row % 8 < 4), 1.0, 0.0)
    pick_g = jnp.where(hit & (row % 8 >= 4), 1.0, 0.0).astype(BF16)
    lane, head_of, piece = stat_lanes((64, HEAD_WIDTH))
    pick_q_low = pick_q.astype(BF16)
    for half in range(2):
        lanes = slice(half * STATS, (half + 1) * STATS)
        both = dot(pick_q_low, q_ref[:, lanes], 1, 0) + dot(pick_g, g_ref[:, lanes], 1, 0)
        out_ref[:, half, :, 0:STATS] = both.reshape(8, 8, STATS).astype(BF16)
        product = dot(pick_q_low, o_ref[:, lanes], 1, 0) * dot(pick_q_low, g_ref[:, lanes], 1, 0)
        stat = jnp.zeros((64, HEAD_WIDTH), F32)
        for inner in range(GROUP):
            mine = head_of == inner
            part = product[:, inner * HEAD_WIDTH : (inner + 1) * HEAD_WIDTH]
            delta = jnp.sum(part, axis=1, keepdims=True)
            norm = norm_ref[half * GROUP + inner : half * GROUP + inner + 1, :]
            norm = jnp.sum(pick_q * norm, axis=1, keepdims=True) * math.sqrt(HEAD_WIDTH)
            stat = jnp.where(mine & (lane < 3 * GROUP), norm, stat)
            stat = jnp.where(mine & (lane >= 3 * GROUP) & (lane < 6 * GROUP), delta, stat)
        high = stat.astype(BF16).astype(F32)
        middle = (stat - high).astype(BF16).astype(F32)
        low = stat - high - middle
        stat = jnp.where(piece == 0, high, jnp.where(piece == 1, middle, low))
        stat = jnp.where(lane == 6 * GROUP, live.astype(F32), stat)
        out_ref[:, half, :, STATS:] = stat.reshape(8, 8, HEAD_WIDTH).astype(BF16)


def compact_kernel(dest_ref, rows_ref, out_ref):
    total = out_ref.shape[1]
    dest = dest_ref[0:1, :]
    hit = lax.broadcasted_iota(jnp.int32, (total, dest.shape[1]), 0) == dest
    rows = rows_ref[...].reshape(dest.shape[1], -1)
    rows = dot(jnp.where(hit, 1.0, 0.0).astype(BF16), rows, 1, 0).astype(BF16)
    for copy in range(out_ref.shape[0]):
        out_ref[copy] = rows


def prompt_kernel(
    in_slot_ref, out_slot_ref, kv_ref, rows_ref, kvg_ref, gq_ref, q_scr, g_scr, acc_ref, back_ref
):
    step = pl.program_id(0)

    @pl.when(step == 0)
    def _():
        acc_ref[...] = jnp.zeros_like(acc_ref)
        slot = in_slot_ref[0:1, :]
        hit = lax.broadcasted_iota(jnp.int32, (2 * LIVE, slot.shape[1]), 0) == slot
        pick = jnp.where(hit, 1.0, 0.0).astype(BF16)
        rows = dot(pick, rows_ref[...].reshape(slot.shape[1], -1), 1, 0).astype(BF16)
        lane, head_of, _ = stat_lanes((LIVE, HEAD_WIDTH))
        stats = rows[0:LIVE, STATS:]
        zero = jnp.zeros((), BF16)
        for head in range(GROUP):
            place = slice(head * LIVE, (head + 1) * LIVE)
            lanes = slice(head * HEAD_WIDTH, (head + 1) * HEAD_WIDTH)
            mine = head_of == head
            q_scr[place, 0:HEAD_WIDTH] = rows[0:LIVE, lanes]
            q_scr[place, HEAD_WIDTH:] = jnp.where(mine & (lane < 3 * GROUP), stats, zero)
            g_scr[place, 0:HEAD_WIDTH] = rows[LIVE:, lanes]
            g_scr[place, HEAD_WIDTH:] = jnp.where(
                mine & (lane >= 3 * GROUP) & (lane < 6 * GROUP), stats, zero
            )
        q_scr[GROUP * LIVE :, :] = jnp.zeros((1024 - GROUP * LIVE, 2 * HEAD_WIDTH), BF16)
        g_scr[GROUP * LIVE :, :] = jnp.zeros((1024 - GROUP * LIVE, 2 * HEAD_WIDTH), BF16)

    keys = kv_ref[:, 0:128, :].reshape(-1, HEAD_WIDTH)
    values = kv_ref[:, 128:256, :].reshape(-1, HEAD_WIDTH)
    lane = lax.broadcasted_iota(jnp.int32, keys.shape, 1)
    minus = jnp.where(lane < 6 * GROUP, -1.0, 0.0).astype(BF16)
    wide_keys = jnp.concatenate([keys, minus], axis=1)
    wide_values = jnp.concatenate([values, minus], axis=1)
    gk = jnp.zeros(keys.shape, F32)
    gv = jnp.zeros(keys.shape, F32)
    for part in range(4):
        rows = slice(256 * part, 256 * part + 256)
        prob = jnp.exp(dot(wide_keys, q_scr[rows, :], 1, 1) * SCALE)
        sgrad = (prob * dot(wide_values, g_scr[rows, :], 1, 1)).astype(BF16)
        gv = gv + dot(prob.astype(BF16), g_scr[rows, 0:HEAD_WIDTH], 1, 0)
        gk = gk + dot(sgrad, q_scr[rows, 0:HEAD_WIDTH], 1, 0)
        acc_ref[rows, :] += dot(sgrad, keys, 0, 0)
    kvg_ref[:, 0:128, :] = (gk * SCALE).astype(BF16).reshape(-1, 128, HEAD_WIDTH)
    kvg_ref[:, 128:256, :] = gv.astype(BF16).reshape(-1, 128, HEAD_WIDTH)

    @pl.when(step == pl.num_programs(0) - 1)
    def _():
        back_ref[...] = jnp.zeros_like(back_ref)
        for head in range(GROUP):
            lanes = slice(head % 4 * HEAD_WIDTH, (head % 4 + 1) * HEAD_WIDTH)
            part = (acc_ref[head * LIVE : (head + 1) * LIVE, :] * SCALE).astype(BF16)
            back_ref[head // 4 * LIVE : (head // 4 + 1) * LIVE, lanes] = part
        slot = out_slot_ref[0:1, :]
        hit = lax.broadcasted_iota(jnp.int32, (2 * LIVE, slot.shape[1]), 0) == slot
        pick = jnp.where(hit, 1.0, 0.0).astype(BF16)
        gq_ref[...] = dot(pick, back_ref[...], 0, 0).reshape(gq_ref.shape).astype(BF16)


def prompt_terms(in_slot, out_slot, kv, rows):
    sources = kv.shape[0]
    per = 2
    block = pl.BlockSpec((per, 256, HEAD_WIDTH), lambda k: (k, 0, 0))
    return pl.pallas_call(
        prompt_kernel,
        grid=(sources // per,),
        in_specs=[
            pl.BlockSpec(in_slot.shape, lambda k: (0, 0)),
            pl.BlockSpec(out_slot.shape, lambda k: (0, 0)),
            block,
            pl.BlockSpec(rows.shape, lambda k: (0, 0, 0)),
        ],
        out_specs=[block, pl.BlockSpec((128, 8, 512), lambda k: (0, 0, 0))],
        out_shape=[
            jax.ShapeDtypeStruct(kv.shape, BF16),
            jax.ShapeDtypeStruct((128, 8, 512), BF16),
        ],
        scratch_shapes=[
            pltpu.VMEM((1024, 2 * HEAD_WIDTH), BF16),
            pltpu.VMEM((1024, 2 * HEAD_WIDTH), BF16),
            pltpu.VMEM((1024, HEAD_WIDTH), F32),
            pltpu.VMEM((2 * LIVE, 512), BF16),
        ],
        interpret=INTERPRET,
    )(in_slot, out_slot, kv, rows)


def final_kernel(parts_ref, own_ref, out_ref, sum_ref):
    for half in range(2):
        for p in range(CLASSES):
            total = parts_ref[half * 8 + p].astype(F32)
            for z in range(1, 8):
                total = total + parts_ref[z * 16 + half * 8 + p].astype(F32)
            for head in range(GROUP):
                rows = slice(head // 4 * 4, head // 4 * 4 + 4)
                part = total[rows, head % 4 * HEAD_WIDTH : (head % 4 + 1) * HEAD_WIDTH]
                first = (half * GROUP + head) * 32 + p
                sum_ref[pl.ds(first, 4, stride=8), :] = part
    for head in range(2 * GROUP):
        lanes = slice(head * HEAD_WIDTH, (head + 1) * HEAD_WIDTH)
        out_ref[:, lanes] = (sum_ref[head * 32 : head * 32 + 32, :] + own_ref[:, lanes]).astype(BF16)


def key_sum_kernel(parts_ref, k_ref, v_ref):
    for head in range(2):
        total = parts_ref[head, 0].astype(F32)
        for k in range(1, parts_ref.shape[1]):
            total = total + parts_ref[head, k].astype(F32)
        lanes = slice(head * HEAD_WIDTH, (head + 1) * HEAD_WIDTH)
        k_ref[:, lanes] = total[0:128].astype(BF16)
        v_ref[:, lanes] = total[128:256].astype(BF16)


def self_kernel(
    info, q_ref, g_ref, norm_ref, delta_ref, col_norm_ref, col_delta_ref, own_ref, kv_ref,
    gk_ref, gv_ref, gq_ref,
):
    p, live = info[0], info[1]
    rows_total = q_ref.shape[0]
    i_row = lax.broadcasted_iota(jnp.int32, (32, rows_total), 1)
    j_row = lax.broadcasted_iota(jnp.int32, (32, rows_total), 0) + p * 32
    live_row = lax.broadcasted_iota(jnp.int32, (rows_total, HEAD_WIDTH), 0) < live
    live_own = lax.broadcasted_iota(jnp.int32, (32, HEAD_WIDTH), 0) + p * 32 < live
    zero = jnp.zeros((), BF16)
    for kv in range(2):
        key_lanes = slice(kv * HEAD_WIDTH, (kv + 1) * HEAD_WIDTH)
        value_lanes = slice((kv + 2) * HEAD_WIDTH, (kv + 3) * HEAD_WIDTH)
        keys, values = own_ref[:, key_lanes], own_ref[:, value_lanes]
        all_keys = kv_ref[:, :, key_lanes].reshape(rows_total, HEAD_WIDTH)
        all_values = kv_ref[:, :, value_lanes].reshape(rows_total, HEAD_WIDTH)
        gk = jnp.zeros((32, HEAD_WIDTH), F32)
        gv = jnp.zeros((32, HEAD_WIDTH), F32)
        for inner in range(GROUP):
            head = kv * GROUP + inner
            lanes = slice(head * HEAD_WIDTH, (head + 1) * HEAD_WIDTH)
            q = q_ref[:, lanes]
            g = jnp.where(live_row, g_ref[:, lanes], zero)
            prob = jnp.exp(dot(keys, q, 1, 1) * SCALE - norm_ref[head : head + 1, :])
            prob = jnp.where(j_row <= i_row, prob, 0.0)
            sgrad = prob * (dot(values, g, 1, 1) - delta_ref[head : head + 1, :])
            gv = gv + dot(prob.astype(BF16), g, 1, 0)
            gk = gk + dot(sgrad.astype(BF16), q, 1, 0)
            q_own = q_ref[pl.ds(pl.multiple_of(p * 32, 32), 32), lanes]
            g_own = g_ref[pl.ds(pl.multiple_of(p * 32, 32), 32), lanes]
            g_own = jnp.where(live_own, g_own, zero)
            prob = jnp.exp(dot(q_own, all_keys, 1, 1) * SCALE - col_norm_ref[:, head : head + 1])
            i_own = lax.broadcasted_iota(jnp.int32, prob.shape, 0) + p * 32
            prob = jnp.where(lax.broadcasted_iota(jnp.int32, prob.shape, 1) <= i_own, prob, 0.0)
            sgrad = prob * (dot(g_own, all_values, 1, 1) - col_delta_ref[:, head : head + 1])
            gq_ref[:, lanes] = dot(sgrad.astype(BF16), all_keys, 1, 0) * SCALE
        gk_ref[:, key_lanes] = (gk * SCALE).astype(BF16)
        gv_ref[:, key_lanes] = gv.astype(BF16)


def shards(
    queries,
    outputs,
    grad_out,
    log_norms,
    lengths,
    prompt_key_rows,
    prompt_value_rows,
    slice_key_rows,
    slice_value_rows,
):
    z = lax.axis_index("sample_0")
    half = lax.axis_index("sample_1")
    p = lax.axis_index("span")
    sample = 2 * z + half
    spans = lax.axis_size("span")
    slice_rows = queries.shape[1]
    heads = queries.shape[2] // HEAD_WIDTH
    class_rows = slice_rows // CLASSES
    q, o, g = queries[0], outputs[0], grad_out[0]
    norms = log_norms[0]
    live = lengths[0]
    smem, vmem = pl.BlockSpec(memory_space=pltpu.SMEM), pl.BlockSpec(memory_space=pltpu.VMEM)

    kv_heads = jnp.concatenate(
        [
            prompt_key_rows.reshape(-1, 2, HEAD_WIDTH).transpose(1, 0, 2),
            prompt_value_rows.reshape(-1, 2, HEAD_WIDTH).transpose(1, 0, 2),
        ],
        axis=1,
    )
    kv_send = jnp.broadcast_to(kv_heads[:, None], (2, spans, *kv_heads.shape[1:]))
    kv = exchange(kv_send.reshape(2 * spans, *kv_heads.shape[1:]), PLANE)

    picked = call(
        pick_kernel,
        jax.ShapeDtypeStruct((8, 2, 8, 1024), BF16),
        jnp.stack([p, sample % 8, live]),
        q,
        o,
        g,
        norms,
        in_specs=[smem] + [vmem] * 4,
    )
    arrived = exchange(picked.reshape(16, 8, 1024), SAMPLE)

    all_lengths = arrived[:, 0, STATS + 6 * GROUP].astype(jnp.int32)
    live_of = jnp.clip((all_lengths - p + CLASSES - 1) // CLASSES, 0, class_rows)
    every_sample = jnp.arange(16)
    first = (jnp.arange(8)[None, :] - every_sample[:, None]) % 8
    held = jnp.clip((live_of[:, None] - first + 7) // 8, 0, 4)
    earlier = (every_sample[None, :] < every_sample[:, None])[:, :, None]
    before = jnp.sum(jnp.where(earlier, held[None], 0), axis=1)
    total = jnp.sum(held, axis=0)
    base = jnp.sum(jnp.where(jnp.arange(8)[None, :] < jnp.arange(8)[:, None], total[None], 0), axis=1)
    mine = jnp.arange(8)[None, :] == z
    own_held = jnp.sum(jnp.where(mine, held, 0), axis=1)
    own_before = jnp.sum(jnp.where(mine, before, 0), axis=1)
    step4 = jnp.arange(4)[None, :]
    compact_slot = jnp.where(step4 < own_held[:, None], own_before[:, None] + step4, -SLOTS)
    compact_dest = compact_slot[:, None, :] + SLOTS * jnp.arange(2)[None, :, None]
    compact_dest = jnp.where(compact_slot[:, None, :] < 0, -1, compact_dest)
    compact = call(
        compact_kernel,
        jax.ShapeDtypeStruct((8, 2 * SLOTS, 1024), BF16),
        compact_dest.reshape(1, 128),
        arrived,
    )
    rows = exchange(compact, "sample_0")
    step = jnp.arange(SLOTS)[None, :]
    in_slot = base[:, None] + step
    in_slot = in_slot[:, None, :] + LIVE * jnp.arange(2)[None, :, None]
    in_slot = jnp.where((step < total[:, None])[:, None, :], in_slot, -1).reshape(1, 16 * SLOTS)
    k = jnp.arange(class_rows)
    holder = (k[None, :] + every_sample[:, None]) % 8
    chosen = holder[:, :, None] == jnp.arange(8)[None, None, :]
    slot_of = jnp.sum(jnp.where(chosen, (base[None, :] + before)[:, None, :], 0), axis=2)
    slot_of = jnp.where(k[None, :] < live_of[:, None], slot_of + k[None, :] // 8, -LIVE * 2)
    out_slot = slot_of.reshape(16, spans, 1, 4) + LIVE * jnp.arange(2)[None, None, :, None]
    out_slot = out_slot.reshape(1, 1024)

    live_rows = lax.broadcasted_iota(jnp.int32, (slice_rows, 1), 0) < live
    g_live = jnp.where(live_rows, g, jnp.zeros((), BF16))
    delta = jnp.sum(
        (g_live.astype(F32) * o.astype(F32)).reshape(slice_rows, heads, HEAD_WIDTH), axis=-1
    ).T
    own_kv = jnp.concatenate([slice_key_rows[0], slice_value_rows[0]], axis=1)
    slice_kv = exchange(jnp.broadcast_to(own_kv[None], (spans, *own_kv.shape)), "span")
    own_rows = slice_rows // spans
    col_norms = lax.dynamic_slice_in_dim(norms, p * own_rows, own_rows, 1).T
    col_delta = lax.dynamic_slice_in_dim(delta, p * own_rows, own_rows, 1).T
    own_shape = jax.ShapeDtypeStruct((own_rows, 2 * HEAD_WIDTH), BF16)
    gk_self, gv_self, gq_self = call(
        self_kernel,
        [own_shape, own_shape, jax.ShapeDtypeStruct((own_rows, heads * HEAD_WIDTH), F32)],
        jnp.stack([p, live]),
        q,
        g,
        norms,
        delta,
        col_norms,
        col_delta,
        own_kv,
        slice_kv,
        in_specs=[smem] + [vmem] * 8,
    )

    kv_grads, gq_parts = prompt_terms(in_slot, out_slot, kv, rows)
    gq_parts = exchange(gq_parts, SAMPLE_SPAN)
    kv_parts = exchange(kv_grads, PLANE)
    prompt_shape = jax.ShapeDtypeStruct(prompt_key_rows.shape, BF16)
    gk_prompt, gv_prompt = call(
        key_sum_kernel,
        [prompt_shape, prompt_shape],
        kv_parts.reshape(2, spans, *kv_parts.shape[1:]),
    )
    grad_query = call(
        final_kernel,
        jax.ShapeDtypeStruct((own_rows, heads * HEAD_WIDTH), BF16),
        gq_parts,
        gq_self,
        scratch_shapes=[pltpu.VMEM((heads * own_rows, HEAD_WIDTH), F32)],
    )
    return grad_query[None], gk_prompt, gv_prompt, gk_self[None], gv_self[None]


def solution(mesh):
    split = Mesh(
        mesh.devices.reshape(8, 2, mesh.shape["span"], mesh.shape["kvhead"]),
        ("sample_0", "sample_1", "span", "kvhead"),
    )
    placed = (
        P(SAMPLE, None, "kvhead"),
        P(SAMPLE, None, "kvhead"),
        P(SAMPLE, None, "kvhead"),
        P(SAMPLE, "kvhead", None),
        P(SAMPLE),
        P(SAMPLE_SPAN, "kvhead"),
        P(SAMPLE_SPAN, "kvhead"),
        P(SAMPLE, "span", "kvhead"),
        P(SAMPLE, "span", "kvhead"),
    )
    return jax.shard_map(
        shards,
        mesh=split,
        in_specs=placed,
        out_specs=(
            P(SAMPLE, "span", "kvhead"),
            P(SAMPLE_SPAN, "kvhead"),
            P(SAMPLE_SPAN, "kvhead"),
            P(SAMPLE, "span", "kvhead"),
            P(SAMPLE, "span", "kvhead"),
        ),
        check_vma=False,
    )
```

```python
import math

import jax
import jax.numpy as jnp
from jax import lax
from jax.experimental import pallas as pl
from jax.experimental.pallas import tpu as pltpu
from jax.sharding import Mesh
from jax.sharding import PartitionSpec as P

HEAD_WIDTH = 128
SAMPLE = ("sample_0", "sample_1")
SPAN = ("span_0", "span_1")
SAMPLE_SPAN = SAMPLE + SPAN
ALONG_X, ALONG_Y = "span_0", ("sample_1", "span_1")
GROUP = 7
CLASSES = 8
SLOTS = 24
LIVE = 144
STATS = GROUP * HEAD_WIDTH
INTERPRET = False
BF16 = jnp.bfloat16
F32 = jnp.float32
SCALE = 1.0 / math.sqrt(HEAD_WIDTH)
EXACT = lax.Precision.HIGHEST


def exchange(tiles, axes):
    return lax.all_to_all(tiles, axes, split_axis=0, concat_axis=0, tiled=True)


def dot(a, b, ca, cb):
    return lax.dot_general(a, b, (((ca,), (cb,)), ((), ())), preferred_element_type=F32)


def call(body, out_shape, *args, **kw):
    return pl.pallas_call(body, out_shape=out_shape, interpret=INTERPRET, **kw)(*args)


def stat_lanes(shape):
    lane = lax.broadcasted_iota(jnp.int32, shape, 1)
    group = jnp.zeros(shape, jnp.int32)
    for edge in range(GROUP, 6 * GROUP, GROUP):
        group = group + jnp.where(lane >= edge, 1, 0)
    piece = jnp.where(group >= 3, group - 3, group)
    return lane, lane - GROUP * group, piece


def pick_kernel(info, q_ref, o_ref, g_ref, norm_ref, out_ref):
    p, turn, live = info[0], info[1], info[2]
    row = lax.broadcasted_iota(jnp.int32, (64, 256), 0)
    i = lax.broadcasted_iota(jnp.int32, (64, 256), 1)
    hit = (i % 8 == p) & (i < live) & ((turn + i // 8) % 8 == row // 8) & (i // 64 == row % 4)
    pick_q = jnp.where(hit & (row % 8 < 4), 1.0, 0.0)
    pick_g = jnp.where(hit & (row % 8 >= 4), 1.0, 0.0).astype(BF16)
    lane, head_of, piece = stat_lanes((64, HEAD_WIDTH))
    pick_q_low = pick_q.astype(BF16)
    for half in range(2):
        lanes = slice(half * STATS, (half + 1) * STATS)
        both = dot(pick_q_low, q_ref[:, lanes], 1, 0) + dot(pick_g, g_ref[:, lanes], 1, 0)
        out_ref[:, half, :, 0:STATS] = both.reshape(8, 8, STATS).astype(BF16)
        product = dot(pick_q_low, o_ref[:, lanes], 1, 0) * dot(pick_q_low, g_ref[:, lanes], 1, 0)
        stat = jnp.zeros((64, HEAD_WIDTH), F32)
        for inner in range(GROUP):
            mine = head_of == inner
            part = product[:, inner * HEAD_WIDTH : (inner + 1) * HEAD_WIDTH]
            delta = jnp.sum(part, axis=1, keepdims=True)
            norm = norm_ref[half * GROUP + inner : half * GROUP + inner + 1, :]
            norm = jnp.sum(pick_q * norm, axis=1, keepdims=True) * math.sqrt(HEAD_WIDTH)
            stat = jnp.where(mine & (lane < 3 * GROUP), norm, stat)
            stat = jnp.where(mine & (lane >= 3 * GROUP) & (lane < 6 * GROUP), delta, stat)
        high = stat.astype(BF16).astype(F32)
        middle = (stat - high).astype(BF16).astype(F32)
        low = stat - high - middle
        stat = jnp.where(piece == 0, high, jnp.where(piece == 1, middle, low))
        stat = jnp.where(lane == 6 * GROUP, live.astype(F32), stat)
        out_ref[:, half, :, STATS:] = stat.reshape(8, 8, HEAD_WIDTH).astype(BF16)


def compact_kernel(dest_ref, rows_ref, out_ref):
    total = out_ref.shape[1]
    dest = dest_ref[0:1, :]
    hit = lax.broadcasted_iota(jnp.int32, (total, dest.shape[1]), 0) == dest
    rows = rows_ref[...].reshape(dest.shape[1], -1)
    rows = dot(jnp.where(hit, 1.0, 0.0).astype(BF16), rows, 1, 0).astype(BF16)
    for copy in range(out_ref.shape[0]):
        out_ref[copy] = rows


def prompt_kernel(in_slot_ref, out_slot_ref, rows_ref, *refs):
    kv_refs, kvg_refs = refs[0:4], refs[4:8]
    gq_ref, q_scr, g_scr, acc_ref, back_ref = refs[8:]
    if True:
        acc_ref[...] = jnp.zeros_like(acc_ref)
        slot = in_slot_ref[0:1, :]
        hit = lax.broadcasted_iota(jnp.int32, (2 * LIVE, slot.shape[1]), 0) == slot
        pick = jnp.where(hit, 1.0, 0.0).astype(BF16)
        rows = dot(pick, rows_ref[...].reshape(slot.shape[1], -1), 1, 0).astype(BF16)
        lane, head_of, _ = stat_lanes((LIVE, HEAD_WIDTH))
        stats = rows[0:LIVE, STATS:]
        zero = jnp.zeros((), BF16)
        for head in range(GROUP):
            place = slice(head * LIVE, (head + 1) * LIVE)
            lanes = slice(head * HEAD_WIDTH, (head + 1) * HEAD_WIDTH)
            mine = head_of == head
            q_scr[place, 0:HEAD_WIDTH] = rows[0:LIVE, lanes]
            q_scr[place, HEAD_WIDTH:] = jnp.where(mine & (lane < 3 * GROUP), stats, zero)
            g_scr[place, 0:HEAD_WIDTH] = rows[LIVE:, lanes]
            g_scr[place, HEAD_WIDTH:] = jnp.where(
                mine & (lane >= 3 * GROUP) & (lane < 6 * GROUP), stats, zero
            )
        q_scr[GROUP * LIVE :, :] = jnp.zeros((1024 - GROUP * LIVE, 2 * HEAD_WIDTH), BF16)
        g_scr[GROUP * LIVE :, :] = jnp.zeros((1024 - GROUP * LIVE, 2 * HEAD_WIDTH), BF16)

    lane = lax.broadcasted_iota(jnp.int32, (256, HEAD_WIDTH), 1)
    minus = jnp.where(lane < 6 * GROUP, -1.0, 0.0).astype(BF16)

    def block(kv_ref, kvg_ref, pair):
        def piece(k):
            return pl.ds(pl.multiple_of(pair * 512 + k * 128, 128), 128)

        keys = jnp.concatenate([kv_ref[piece(0), :], kv_ref[piece(2), :]], axis=0)
        values = jnp.concatenate([kv_ref[piece(1), :], kv_ref[piece(3), :]], axis=0)
        wide_keys = jnp.concatenate([keys, minus], axis=1)
        wide_values = jnp.concatenate([values, minus], axis=1)
        gk = jnp.zeros(keys.shape, F32)
        gv = jnp.zeros(keys.shape, F32)
        for part in range(4):
            rows = slice(256 * part, 256 * part + 256)
            prob = jnp.exp(dot(wide_keys, q_scr[rows, :], 1, 1) * SCALE)
            sgrad = (prob * dot(wide_values, g_scr[rows, :], 1, 1)).astype(BF16)
            gv = gv + dot(prob.astype(BF16), g_scr[rows, 0:HEAD_WIDTH], 1, 0)
            gk = gk + dot(sgrad, q_scr[rows, 0:HEAD_WIDTH], 1, 0)
            acc_ref[rows, :] += dot(sgrad, keys, 0, 0)
        gk, gv = (gk * SCALE).astype(BF16), gv.astype(BF16)
        for k, part in enumerate((gk[0:128], gv[0:128], gk[128:256], gv[128:256])):
            kvg_ref[piece(k), :] = part

    for kv_ref, kvg_ref in zip(kv_refs, kvg_refs):
        lax.fori_loop(0, 2, lambda k, _: block(kv_ref, kvg_ref, k), None)

    if True:
        back_ref[...] = jnp.zeros_like(back_ref)
        for head in range(GROUP):
            lanes = slice(head % 4 * HEAD_WIDTH, (head % 4 + 1) * HEAD_WIDTH)
            part = (acc_ref[head * LIVE : (head + 1) * LIVE, :] * SCALE).astype(BF16)
            back_ref[head // 4 * LIVE : (head // 4 + 1) * LIVE, lanes] = part
        slot = out_slot_ref[0:1, :]
        hit = lax.broadcasted_iota(jnp.int32, (2 * LIVE, slot.shape[1]), 0) == slot
        pick = jnp.where(hit, 1.0, 0.0).astype(BF16)
        gq_ref[...] = dot(pick, back_ref[...], 0, 0).reshape(gq_ref.shape).astype(BF16)


def prompt_terms(in_slot, out_slot, rows, *kv):
    *kv_grads, gq = call(
        prompt_kernel,
        [jax.ShapeDtypeStruct((1024, HEAD_WIDTH), BF16)] * 4
        + [jax.ShapeDtypeStruct((128, 8, 512), BF16)],
        in_slot,
        out_slot,
        rows,
        *kv,
        scratch_shapes=[
            pltpu.VMEM((1024, 2 * HEAD_WIDTH), BF16),
            pltpu.VMEM((1024, 2 * HEAD_WIDTH), BF16),
            pltpu.VMEM((1024, HEAD_WIDTH), F32),
            pltpu.VMEM((2 * LIVE, 512), BF16),
        ],
    )
    return kv_grads, gq


def final_kernel(parts_ref, own_ref, out_ref, sum_ref):
    for half in range(2):
        for p in range(CLASSES):
            total = parts_ref[half * 8 + p].astype(F32)
            for z in range(1, 8):
                total = total + parts_ref[z * 16 + half * 8 + p].astype(F32)
            for head in range(GROUP):
                rows = slice(head // 4 * 4, head // 4 * 4 + 4)
                part = total[rows, head % 4 * HEAD_WIDTH : (head % 4 + 1) * HEAD_WIDTH]
                first = (half * GROUP + head) * 32 + p
                sum_ref[pl.ds(first, 4, stride=8), :] = part
    for head in range(2 * GROUP):
        lanes = slice(head * HEAD_WIDTH, (head + 1) * HEAD_WIDTH)
        out_ref[:, lanes] = (sum_ref[head * 32 : head * 32 + 32, :] + own_ref[:, lanes]).astype(BF16)


def pack_kernel(info, pk_ref, pv_ref, sk_ref, sv_ref, own_ref, other_ref):
    half = info[0]
    low, high = slice(0, HEAD_WIDTH), slice(HEAD_WIDTH, 2 * HEAD_WIDTH)
    for k, ref in enumerate((pk_ref, pv_ref)):
        rows = slice(128 * k, 128 * k + 128)
        own_ref[rows, :] = jnp.where(half == 0, ref[:, low], ref[:, high])
        other_ref[rows, :] = jnp.where(half == 0, ref[:, high], ref[:, low])
    for k, (ref, lanes) in enumerate(((sk_ref, low), (sk_ref, high), (sv_ref, low), (sv_ref, high))):
        own_ref[256 + 32 * k : 288 + 32 * k, :] = ref[:, lanes]


def x_sum_kernel(a_ref, b_ref, c_ref, d_ref, *out_refs):
    for k, out_ref in enumerate(out_refs):
        rows = slice(256 * k, 256 * k + 256)
        total = a_ref[rows, :].astype(F32) + b_ref[rows, :].astype(F32)
        total = total + c_ref[rows, :].astype(F32) + d_ref[rows, :].astype(F32)
        out_ref[...] = total.astype(BF16)


def y_sum_kernel(info, a_ref, b_ref, c_ref, d_ref, k_ref, v_ref):
    half = info[0]
    own = a_ref[...].astype(F32) + b_ref[...].astype(F32)
    other = c_ref[...].astype(F32) + d_ref[...].astype(F32)
    low = jnp.where(half == 0, own, other).astype(BF16)
    high = jnp.where(half == 0, other, own).astype(BF16)
    for k, ref in enumerate((k_ref, v_ref)):
        ref[:, 0:HEAD_WIDTH] = low[128 * k : 128 * k + 128]
        ref[:, HEAD_WIDTH:] = high[128 * k : 128 * k + 128]


def shifted(value, by):
    return lax.ppermute(value, ALONG_X, [(k, (k + by) % 4) for k in range(4)])


def crossed(value, by):
    return lax.ppermute(value, ALONG_Y, [(k, k ^ by) for k in range(4)])


def self_kernel(
    info, q_ref, g_ref, norm_ref, delta_ref, col_norm_ref, col_delta_ref, kv0_ref, kv1_ref, kv2_ref,
    kv3_ref, gk_ref, gv_ref, gq_ref,
):
    p, live = info[0], info[1]
    rows_total = q_ref.shape[0]
    i_row = lax.broadcasted_iota(jnp.int32, (32, rows_total), 1)
    j_row = lax.broadcasted_iota(jnp.int32, (32, rows_total), 0) + p * 32
    live_row = lax.broadcasted_iota(jnp.int32, (rows_total, HEAD_WIDTH), 0) < live
    live_own = lax.broadcasted_iota(jnp.int32, (32, HEAD_WIDTH), 0) + p * 32 < live
    zero = jnp.zeros((), BF16)
    kv_refs = (kv0_ref, kv1_ref, kv2_ref, kv3_ref)
    lane = lax.broadcasted_iota(jnp.int32, (1, rows_total), 1)
    block = lane // 32
    from_span = (p // 2 + 4 - block // 2) % 4 * 2 + (p % 2 + block % 2) % 2
    position = from_span * 32 + lane % 32
    for kv in range(2):
        key_lanes = slice(kv * HEAD_WIDTH, (kv + 1) * HEAD_WIDTH)

        def piece(ref, which, kind):
            first = 1024 + 128 * which + 32 * (2 * kind + kv)
            return ref[first : first + 32, :]

        keys, values = piece(kv0_ref, 0, 0), piece(kv0_ref, 0, 1)
        all_keys = jnp.concatenate([piece(r, w, 0) for r in kv_refs for w in range(2)], axis=0)
        all_values = jnp.concatenate([piece(r, w, 1) for r in kv_refs for w in range(2)], axis=0)
        gk = jnp.zeros((32, HEAD_WIDTH), F32)
        gv = jnp.zeros((32, HEAD_WIDTH), F32)
        for inner in range(GROUP):
            head = kv * GROUP + inner
            lanes = slice(head * HEAD_WIDTH, (head + 1) * HEAD_WIDTH)
            q = q_ref[:, lanes]
            g = jnp.where(live_row, g_ref[:, lanes], zero)
            prob = jnp.exp(dot(keys, q, 1, 1) * SCALE - norm_ref[head : head + 1, :])
            prob = jnp.where(j_row <= i_row, prob, 0.0)
            sgrad = prob * (dot(values, g, 1, 1) - delta_ref[head : head + 1, :])
            gv = gv + dot(prob.astype(BF16), g, 1, 0)
            gk = gk + dot(sgrad.astype(BF16), q, 1, 0)
            q_own = q_ref[pl.ds(pl.multiple_of(p * 32, 32), 32), lanes]
            g_own = g_ref[pl.ds(pl.multiple_of(p * 32, 32), 32), lanes]
            g_own = jnp.where(live_own, g_own, zero)
            prob = jnp.exp(dot(q_own, all_keys, 1, 1) * SCALE - col_norm_ref[:, head : head + 1])
            i_own = lax.broadcasted_iota(jnp.int32, prob.shape, 0) + p * 32
            prob = jnp.where(position <= i_own, prob, 0.0)
            sgrad = prob * (dot(g_own, all_values, 1, 1) - col_delta_ref[:, head : head + 1])
            gq_ref[:, lanes] = dot(sgrad.astype(BF16), all_keys, 1, 0) * SCALE
        gk_ref[:, key_lanes] = (gk * SCALE).astype(BF16)
        gv_ref[:, key_lanes] = gv.astype(BF16)


def shards(
    queries,
    outputs,
    grad_out,
    log_norms,
    lengths,
    prompt_key_rows,
    prompt_value_rows,
    slice_key_rows,
    slice_value_rows,
):
    z = lax.axis_index("sample_0")
    half = lax.axis_index("sample_1")
    p = lax.axis_index(SPAN)
    sample = 2 * z + half
    spans = lax.axis_size(SPAN)
    slice_rows = queries.shape[1]
    heads = queries.shape[2] // HEAD_WIDTH
    class_rows = slice_rows // CLASSES
    q, o, g = queries[0], outputs[0], grad_out[0]
    norms = log_norms[0]
    live = lengths[0]
    smem, vmem = pl.BlockSpec(memory_space=pltpu.SMEM), pl.BlockSpec(memory_space=pltpu.VMEM)

    packed = lambda rows: jax.ShapeDtypeStruct((rows, HEAD_WIDTH), BF16)
    own, other = call(
        pack_kernel,
        [packed(384), packed(256)],
        half[None],
        prompt_key_rows,
        prompt_value_rows,
        slice_key_rows[0],
        slice_value_rows[0],
        in_specs=[smem] + [vmem] * 4,
    )
    beside = crossed(own, 1)
    column = jnp.concatenate(
        [own[:256], beside[:256], crossed(other, 2), crossed(other, 3), own[256:], beside[256:]]
    )
    kv = [column] + [shifted(column, k) for k in (1, 2, 3)]

    picked = call(
        pick_kernel,
        jax.ShapeDtypeStruct((8, 2, 8, 1024), BF16),
        jnp.stack([p, sample % 8, live]),
        q,
        o,
        g,
        norms,
        in_specs=[smem] + [vmem] * 4,
    )
    arrived = exchange(picked.reshape(16, 8, 1024), SAMPLE)

    all_lengths = arrived[:, 0, STATS + 6 * GROUP].astype(jnp.int32)
    live_of = jnp.clip((all_lengths - p + CLASSES - 1) // CLASSES, 0, class_rows)
    every_sample = jnp.arange(16)
    first = (jnp.arange(8)[None, :] - every_sample[:, None]) % 8
    held = jnp.clip((live_of[:, None] - first + 7) // 8, 0, 4)
    earlier = (every_sample[None, :] < every_sample[:, None])[:, :, None]
    before = jnp.sum(jnp.where(earlier, held[None], 0), axis=1)
    total = jnp.sum(held, axis=0)
    base = jnp.sum(jnp.where(jnp.arange(8)[None, :] < jnp.arange(8)[:, None], total[None], 0), axis=1)
    mine = jnp.arange(8)[None, :] == z
    own_held = jnp.sum(jnp.where(mine, held, 0), axis=1)
    own_before = jnp.sum(jnp.where(mine, before, 0), axis=1)
    step4 = jnp.arange(4)[None, :]
    compact_slot = jnp.where(step4 < own_held[:, None], own_before[:, None] + step4, -SLOTS)
    compact_dest = compact_slot[:, None, :] + SLOTS * jnp.arange(2)[None, :, None]
    compact_dest = jnp.where(compact_slot[:, None, :] < 0, -1, compact_dest)
    compact = call(
        compact_kernel,
        jax.ShapeDtypeStruct((8, 2 * SLOTS, 1024), BF16),
        compact_dest.reshape(1, 128),
        arrived,
    )
    rows = exchange(compact, "sample_0")
    step = jnp.arange(SLOTS)[None, :]
    in_slot = base[:, None] + step
    in_slot = in_slot[:, None, :] + LIVE * jnp.arange(2)[None, :, None]
    in_slot = jnp.where((step < total[:, None])[:, None, :], in_slot, -1).reshape(1, 16 * SLOTS)
    k = jnp.arange(class_rows)
    holder = (k[None, :] + every_sample[:, None]) % 8
    chosen = holder[:, :, None] == jnp.arange(8)[None, None, :]
    slot_of = jnp.sum(jnp.where(chosen, (base[None, :] + before)[:, None, :], 0), axis=2)
    slot_of = jnp.where(k[None, :] < live_of[:, None], slot_of + k[None, :] // 8, -LIVE * 2)
    out_slot = slot_of.reshape(16, spans, 1, 4) + LIVE * jnp.arange(2)[None, None, :, None]
    out_slot = out_slot.reshape(1, 1024)

    live_rows = lax.broadcasted_iota(jnp.int32, (slice_rows, 1), 0) < live
    g_live = jnp.where(live_rows, g, jnp.zeros((), BF16))
    delta = jnp.sum(
        (g_live.astype(F32) * o.astype(F32)).reshape(slice_rows, heads, HEAD_WIDTH), axis=-1
    ).T
    own_rows = slice_rows // spans
    col_norms = lax.dynamic_slice_in_dim(norms, p * own_rows, own_rows, 1).T
    col_delta = lax.dynamic_slice_in_dim(delta, p * own_rows, own_rows, 1).T
    own_shape = jax.ShapeDtypeStruct((own_rows, 2 * HEAD_WIDTH), BF16)
    gk_self, gv_self, gq_self = call(
        self_kernel,
        [own_shape, own_shape, jax.ShapeDtypeStruct((own_rows, heads * HEAD_WIDTH), F32)],
        jnp.stack([p, live]),
        q,
        g,
        norms,
        delta,
        col_norms,
        col_delta,
        *kv,
        in_specs=[smem] + [vmem] * 10,
    )

    kv_grads, gq_parts = prompt_terms(in_slot, out_slot, rows, *kv)
    gq_parts = exchange(gq_parts, SAMPLE_SPAN)
    parts = [kv_grads[0]] + [shifted(kv_grads[k], -k) for k in (1, 2, 3)]
    parts = call(x_sum_kernel, [packed(256)] * 4, *parts)
    parts = [parts[0]] + [crossed(parts[k], k) for k in (1, 2, 3)]
    prompt_shape = jax.ShapeDtypeStruct(prompt_key_rows.shape, BF16)
    gk_prompt, gv_prompt = call(
        y_sum_kernel,
        [prompt_shape, prompt_shape],
        half[None],
        *parts,
        in_specs=[smem] + [vmem] * 4,
    )
    grad_query = call(
        final_kernel,
        jax.ShapeDtypeStruct((own_rows, heads * HEAD_WIDTH), BF16),
        gq_parts,
        gq_self,
        scratch_shapes=[pltpu.VMEM((heads * own_rows, HEAD_WIDTH), F32)],
    )
    return grad_query[None], gk_prompt, gv_prompt, gk_self[None], gv_self[None]


def solution(mesh):
    split = Mesh(
        mesh.devices.reshape(8, 2, 4, 2, mesh.shape["kvhead"]), SAMPLE_SPAN + ("kvhead",)
    )
    placed = (
        P(SAMPLE, None, "kvhead"),
        P(SAMPLE, None, "kvhead"),
        P(SAMPLE, None, "kvhead"),
        P(SAMPLE, "kvhead", None),
        P(SAMPLE),
        P(SAMPLE_SPAN, "kvhead"),
        P(SAMPLE_SPAN, "kvhead"),
        P(SAMPLE, SPAN, "kvhead"),
        P(SAMPLE, SPAN, "kvhead"),
    )
    return jax.shard_map(
        shards,
        mesh=split,
        in_specs=placed,
        out_specs=(
            P(SAMPLE, SPAN, "kvhead"),
            P(SAMPLE_SPAN, "kvhead"),
            P(SAMPLE_SPAN, "kvhead"),
            P(SAMPLE, SPAN, "kvhead"),
            P(SAMPLE, SPAN, "kvhead"),
        ),
        check_vma=False,
    )
```

```python
import math

import jax
import jax.numpy as jnp
from jax import lax
from jax.experimental import pallas as pl
from jax.experimental.pallas import tpu as pltpu
from jax.sharding import Mesh
from jax.sharding import PartitionSpec as P

HEAD_WIDTH = 128
SAMPLE = ("sample_0", "sample_1")
SPAN = ("span_0", "span_1")
SAMPLE_SPAN = SAMPLE + SPAN
ALONG_X, ALONG_Y = "span_0", ("sample_1", "span_1")
GROUP = 7
CLASSES = 8
SLOTS = 24
LIVE = 144
STATS = GROUP * HEAD_WIDTH
INTERPRET = False
VMEM_BYTES = 24 * 1024 * 1024
BF16 = jnp.bfloat16
F32 = jnp.float32
SCALE = 1.0 / math.sqrt(HEAD_WIDTH)


def exchange(tiles, axes):
    return lax.all_to_all(tiles, axes, split_axis=0, concat_axis=0, tiled=True)


def dot(a, b, ca, cb):
    return lax.dot_general(a, b, (((ca,), (cb,)), ((), ())), preferred_element_type=F32)


def call(body, out_shape, *args, **kw):
    params = pltpu.CompilerParams(vmem_limit_bytes=VMEM_BYTES)
    return pl.pallas_call(
        body, out_shape=out_shape, interpret=INTERPRET, compiler_params=params, **kw
    )(*args)


def stat_lanes(shape):
    lane = lax.broadcasted_iota(jnp.int32, shape, 1)
    group = jnp.zeros(shape, jnp.int32)
    for edge in range(GROUP, 6 * GROUP, GROUP):
        group = group + jnp.where(lane >= edge, 1, 0)
    piece = jnp.where(group >= 3, group - 3, group)
    return lane, lane - GROUP * group, piece


def pick_kernel(p_ref, turn_ref, live_ref, q_ref, o_ref, g_ref, norm_ref, out_ref):
    p, turn, live = p_ref[0], turn_ref[0], live_ref[0]
    row = lax.broadcasted_iota(jnp.int32, (64, 256), 0)
    i = lax.broadcasted_iota(jnp.int32, (64, 256), 1)
    hit = (i % 8 == p) & (i < live) & ((turn + i // 8) % 8 == row // 8) & (i // 64 == row % 4)
    pick_q = jnp.where(hit & (row % 8 < 4), 1.0, 0.0)
    pick_g = jnp.where(hit & (row % 8 >= 4), 1.0, 0.0).astype(BF16)
    lane, head_of, piece = stat_lanes((64, HEAD_WIDTH))
    pick_q_low = pick_q.astype(BF16)
    for half in range(2):
        lanes = slice(half * STATS, (half + 1) * STATS)
        both = dot(pick_q_low, q_ref[:, lanes], 1, 0) + dot(pick_g, g_ref[:, lanes], 1, 0)
        out_ref[:, half, :, 0:STATS] = both.reshape(8, 8, STATS).astype(BF16)
        product = dot(pick_q_low, o_ref[:, lanes], 1, 0) * dot(pick_q_low, g_ref[:, lanes], 1, 0)
        stat = jnp.zeros((64, HEAD_WIDTH), F32)
        for inner in range(GROUP):
            mine = head_of == inner
            part = product[:, inner * HEAD_WIDTH : (inner + 1) * HEAD_WIDTH]
            delta = jnp.sum(part, axis=1, keepdims=True)
            norm = norm_ref[half * GROUP + inner]
            norm = jnp.sum(pick_q * norm, axis=1, keepdims=True) * math.sqrt(HEAD_WIDTH)
            stat = jnp.where(mine & (lane < 3 * GROUP), norm, stat)
            stat = jnp.where(mine & (lane >= 3 * GROUP) & (lane < 6 * GROUP), delta, stat)
        high = stat.astype(BF16).astype(F32)
        middle = (stat - high).astype(BF16).astype(F32)
        low = stat - high - middle
        stat = jnp.where(piece == 0, high, jnp.where(piece == 1, middle, low))
        stat = jnp.where(lane == 6 * GROUP, live.astype(F32), stat)
        out_ref[:, half, :, STATS:] = stat.reshape(8, 8, HEAD_WIDTH).astype(BF16)


def compact_kernel(p_ref, z_ref, rows_ref, out_ref):
    rows = rows_ref[...].reshape(128, 1024)
    shape = (128, 128)
    row = lax.broadcasted_iota(jnp.int32, shape, 0)
    col = lax.broadcasted_iota(jnp.int32, shape, 1)
    length = rows[:, STATS + 6 * GROUP : STATS + 6 * GROUP + 1].astype(F32)
    length = jnp.broadcast_to(length, shape).astype(jnp.int32)
    count = (length - p_ref[0] + 7) >> 3
    valid = 8 * (row & 3) + ((z_ref[0] - (row >> 3)) & 7) < count
    earlier = jnp.where(((col >> 3) < (row >> 3)) & (((col >> 2) & 1) == 0), 1.0, 0.0)
    before = dot(earlier.astype(BF16), jnp.where(valid, 1.0, 0.0).astype(BF16), 1, 0)
    place = before.astype(jnp.int32) + (row & 3) + SLOTS * ((row >> 2) & 1)
    pick = jnp.where(valid & (place == col), 1.0, 0.0).astype(BF16)
    rows = dot(pick, rows, 0, 0)[0 : 2 * SLOTS].astype(BF16)
    for copy in range(out_ref.shape[0]):
        out_ref[copy] = rows


def prompt_kernel(in_slot_ref, out_slot_ref, rows_ref, *refs):
    kv_refs, kvg_refs = refs[0:4], refs[4:8]
    gq_ref, q_scr, g_scr, acc_ref, back_ref = refs[8:]
    acc_ref[...] = jnp.zeros_like(acc_ref)
    slot = in_slot_ref[0:1, :]
    hit = lax.broadcasted_iota(jnp.int32, (2 * LIVE, slot.shape[1]), 0) == slot
    pick = jnp.where(hit, 1.0, 0.0).astype(BF16)
    rows = dot(pick, rows_ref[...].reshape(slot.shape[1], -1), 1, 0).astype(BF16)
    lane, head_of, _ = stat_lanes((LIVE, HEAD_WIDTH))
    stats = rows[0:LIVE, STATS:]
    zero = jnp.zeros((), BF16)
    for head in range(GROUP):
        place = slice(head * LIVE, (head + 1) * LIVE)
        lanes = slice(head * HEAD_WIDTH, (head + 1) * HEAD_WIDTH)
        mine = head_of == head
        q_scr[place, 0:HEAD_WIDTH] = rows[0:LIVE, lanes]
        q_scr[place, HEAD_WIDTH:] = jnp.where(mine & (lane < 3 * GROUP), stats, zero)
        g_scr[place, 0:HEAD_WIDTH] = rows[LIVE:, lanes]
        g_scr[place, HEAD_WIDTH:] = jnp.where(
            mine & (lane >= 3 * GROUP) & (lane < 6 * GROUP), stats, zero
        )
    q_scr[GROUP * LIVE :, :] = jnp.zeros((1024 - GROUP * LIVE, 2 * HEAD_WIDTH), BF16)
    g_scr[GROUP * LIVE :, :] = jnp.zeros((1024 - GROUP * LIVE, 2 * HEAD_WIDTH), BF16)

    lane = lax.broadcasted_iota(jnp.int32, (256, HEAD_WIDTH), 1)
    minus = jnp.where(lane < 6 * GROUP, -1.0, 0.0).astype(BF16)

    def block(kv_ref, kvg_ref, pair):
        def piece(k):
            return pl.ds(pl.multiple_of(pair * 512 + k * 128, 128), 128)

        keys = jnp.concatenate([kv_ref[piece(0), :], kv_ref[piece(2), :]], axis=0)
        values = jnp.concatenate([kv_ref[piece(1), :], kv_ref[piece(3), :]], axis=0)
        wide_keys = jnp.concatenate([keys, minus], axis=1)
        wide_values = jnp.concatenate([values, minus], axis=1)
        gk = jnp.zeros(keys.shape, F32)
        gv = jnp.zeros(keys.shape, F32)
        for part in range(4):
            rows = slice(256 * part, 256 * part + 256)
            prob = jnp.exp(dot(wide_keys, q_scr[rows, :], 1, 1) * SCALE)
            sgrad = (prob * dot(wide_values, g_scr[rows, :], 1, 1)).astype(BF16)
            gv = gv + dot(prob.astype(BF16), g_scr[rows, 0:HEAD_WIDTH], 1, 0)
            gk = gk + dot(sgrad, q_scr[rows, 0:HEAD_WIDTH], 1, 0)
            acc_ref[rows, :] += dot(sgrad, keys, 0, 0)
        gk, gv = (gk * SCALE).astype(BF16), gv.astype(BF16)
        for k, part in enumerate((gk[0:128], gv[0:128], gk[128:256], gv[128:256])):
            kvg_ref[piece(k), :] = part

    for kv_ref, kvg_ref in zip(kv_refs, kvg_refs):
        lax.fori_loop(0, 2, lambda k, _: block(kv_ref, kvg_ref, k), None)

    back_ref[...] = jnp.zeros_like(back_ref)
    for head in range(GROUP):
        lanes = slice(head % 4 * HEAD_WIDTH, (head % 4 + 1) * HEAD_WIDTH)
        part = (acc_ref[head * LIVE : (head + 1) * LIVE, :] * SCALE).astype(BF16)
        back_ref[head // 4 * LIVE : (head // 4 + 1) * LIVE, lanes] = part
    slot = out_slot_ref[0:1, :]
    hit = lax.broadcasted_iota(jnp.int32, (2 * LIVE, slot.shape[1]), 0) == slot
    pick = jnp.where(hit, 1.0, 0.0).astype(BF16)
    gq_ref[...] = dot(pick, back_ref[...], 0, 0).reshape(gq_ref.shape).astype(BF16)


def prompt_terms(in_slot, out_slot, rows, *kv):
    *kv_grads, gq = call(
        prompt_kernel,
        [jax.ShapeDtypeStruct((1024, HEAD_WIDTH), BF16)] * 4
        + [jax.ShapeDtypeStruct((128, 8, 512), BF16)],
        in_slot,
        out_slot,
        rows,
        *kv,
        scratch_shapes=[
            pltpu.VMEM((1024, 2 * HEAD_WIDTH), BF16),
            pltpu.VMEM((1024, 2 * HEAD_WIDTH), BF16),
            pltpu.VMEM((1024, HEAD_WIDTH), F32),
            pltpu.VMEM((2 * LIVE, 512), BF16),
        ],
    )
    return kv_grads, gq


def final_kernel(parts_ref, own_ref, out_ref, sum_ref):
    for half in range(2):
        for p in range(CLASSES):
            total = parts_ref[half * 8 + p].astype(F32)
            for z in range(1, 8):
                total = total + parts_ref[z * 16 + half * 8 + p].astype(F32)
            for head in range(GROUP):
                rows = slice(head // 4 * 4, head // 4 * 4 + 4)
                part = total[rows, head % 4 * HEAD_WIDTH : (head % 4 + 1) * HEAD_WIDTH]
                first = (half * GROUP + head) * 32 + p
                sum_ref[pl.ds(first, 4, stride=8), :] = part
    for head in range(2 * GROUP):
        lanes = slice(head * HEAD_WIDTH, (head + 1) * HEAD_WIDTH)
        out_ref[:, lanes] = (sum_ref[head * 32 : head * 32 + 32, :] + own_ref[:, lanes]).astype(BF16)


def pack_kernel(info, pk_ref, pv_ref, sk_ref, sv_ref, own_ref, other_ref):
    half = info[0]
    low, high = slice(0, HEAD_WIDTH), slice(HEAD_WIDTH, 2 * HEAD_WIDTH)
    for k, ref in enumerate((pk_ref, pv_ref)):
        rows = slice(128 * k, 128 * k + 128)
        own_ref[rows, :] = jnp.where(half == 0, ref[:, low], ref[:, high])
        other_ref[rows, :] = jnp.where(half == 0, ref[:, high], ref[:, low])
    for k, (ref, lanes) in enumerate(((sk_ref, low), (sk_ref, high), (sv_ref, low), (sv_ref, high))):
        own_ref[256 + 32 * k : 288 + 32 * k, :] = ref[:, lanes]


def x_sum_kernel(a_ref, b_ref, c_ref, d_ref, *out_refs):
    for k, out_ref in enumerate(out_refs):
        rows = slice(256 * k, 256 * k + 256)
        total = a_ref[rows, :].astype(F32) + b_ref[rows, :].astype(F32)
        total = total + c_ref[rows, :].astype(F32) + d_ref[rows, :].astype(F32)
        out_ref[...] = total.astype(BF16)


def y_sum_kernel(info, a_ref, b_ref, c_ref, d_ref, k_ref, v_ref):
    half = info[0]
    own = a_ref[...].astype(F32) + b_ref[...].astype(F32)
    other = c_ref[...].astype(F32) + d_ref[...].astype(F32)
    low = jnp.where(half == 0, own, other).astype(BF16)
    high = jnp.where(half == 0, other, own).astype(BF16)
    for k, ref in enumerate((k_ref, v_ref)):
        ref[:, 0:HEAD_WIDTH] = low[128 * k : 128 * k + 128]
        ref[:, HEAD_WIDTH:] = high[128 * k : 128 * k + 128]


def shifted(value, by):
    return lax.ppermute(value, ALONG_X, [(k, (k + by) % 4) for k in range(4)])


def crossed(value, by):
    return lax.ppermute(value, ALONG_Y, [(k, k ^ by) for k in range(4)])


def self_kernel(
    p_ref, live_ref, q_ref, g_ref, norm_ref, delta_ref, col_norm_ref, col_delta_ref, kv0_ref, kv1_ref, kv2_ref,
    kv3_ref, gk_ref, gv_ref, gq_ref,
):
    p, live = p_ref[0], live_ref[0]
    rows_total = q_ref.shape[0]
    i_row = lax.broadcasted_iota(jnp.int32, (32, rows_total), 1)
    j_row = lax.broadcasted_iota(jnp.int32, (32, rows_total), 0) + p * 32
    live_row = lax.broadcasted_iota(jnp.int32, (rows_total, HEAD_WIDTH), 0) < live
    live_own = lax.broadcasted_iota(jnp.int32, (32, HEAD_WIDTH), 0) + p * 32 < live
    zero = jnp.zeros((), BF16)
    kv_refs = (kv0_ref, kv1_ref, kv2_ref, kv3_ref)
    lane = lax.broadcasted_iota(jnp.int32, (1, rows_total), 1)
    block = lane // 32
    from_span = (p // 2 + 4 - block // 2) % 4 * 2 + (p % 2 + block % 2) % 2
    position = from_span * 32 + lane % 32
    for kv in range(2):
        key_lanes = slice(kv * HEAD_WIDTH, (kv + 1) * HEAD_WIDTH)

        def piece(ref, which, kind):
            first = 1024 + 128 * which + 32 * (2 * kind + kv)
            return ref[first : first + 32, :]

        keys, values = piece(kv0_ref, 0, 0), piece(kv0_ref, 0, 1)
        all_keys = jnp.concatenate([piece(r, w, 0) for r in kv_refs for w in range(2)], axis=0)
        all_values = jnp.concatenate([piece(r, w, 1) for r in kv_refs for w in range(2)], axis=0)
        gk = jnp.zeros((32, HEAD_WIDTH), F32)
        gv = jnp.zeros((32, HEAD_WIDTH), F32)
        for inner in range(GROUP):
            head = kv * GROUP + inner
            lanes = slice(head * HEAD_WIDTH, (head + 1) * HEAD_WIDTH)
            q = q_ref[:, lanes]
            g = jnp.where(live_row, g_ref[:, lanes], zero)
            prob = jnp.exp(dot(keys, q, 1, 1) * SCALE - norm_ref[head])
            prob = jnp.where(j_row <= i_row, prob, 0.0)
            sgrad = prob * (dot(values, g, 1, 1) - delta_ref[head : head + 1, :])
            gv = gv + dot(prob.astype(BF16), g, 1, 0)
            gk = gk + dot(sgrad.astype(BF16), q, 1, 0)
            q_own = q_ref[pl.ds(pl.multiple_of(p * 32, 32), 32), lanes]
            g_own = g_ref[pl.ds(pl.multiple_of(p * 32, 32), 32), lanes]
            g_own = jnp.where(live_own, g_own, zero)
            prob = jnp.exp(dot(q_own, all_keys, 1, 1) * SCALE - col_norm_ref[:, head : head + 1])
            i_own = lax.broadcasted_iota(jnp.int32, prob.shape, 0) + p * 32
            prob = jnp.where(position <= i_own, prob, 0.0)
            sgrad = prob * (dot(g_own, all_values, 1, 1) - col_delta_ref[:, head : head + 1])
            gq_ref[:, lanes] = dot(sgrad.astype(BF16), all_keys, 1, 0) * SCALE
        gk_ref[:, key_lanes] = (gk * SCALE).astype(BF16)
        gv_ref[:, key_lanes] = gv.astype(BF16)


def shards(
    queries,
    outputs,
    grad_out,
    log_norms,
    lengths,
    prompt_key_rows,
    prompt_value_rows,
    slice_key_rows,
    slice_value_rows,
):
    z = lax.axis_index("sample_0")
    half = lax.axis_index("sample_1")
    p = lax.axis_index(SPAN)
    sample = 2 * z + half
    spans = lax.axis_size(SPAN)
    slice_rows = queries.shape[1]
    heads = queries.shape[2] // HEAD_WIDTH
    class_rows = slice_rows // CLASSES
    q, o, g = queries[0], outputs[0], grad_out[0]
    norms = log_norms.transpose(1, 0, 2)
    live = lengths[0]
    smem, vmem = pl.BlockSpec(memory_space=pltpu.SMEM), pl.BlockSpec(memory_space=pltpu.VMEM)

    picked = call(
        pick_kernel,
        jax.ShapeDtypeStruct((8, 2, 8, 1024), BF16),
        p[None],
        (sample % 8)[None],
        lengths,
        q,
        o,
        g,
        norms,
        in_specs=[smem] * 3 + [vmem] * 4,
    )
    arrived = exchange(picked.reshape(16, 8, 1024), SAMPLE)

    packed = lambda rows: jax.ShapeDtypeStruct((rows, HEAD_WIDTH), BF16)
    own, other = call(
        pack_kernel,
        [packed(384), packed(256)],
        half[None],
        prompt_key_rows,
        prompt_value_rows,
        slice_key_rows[0],
        slice_value_rows[0],
        in_specs=[smem] + [vmem] * 4,
    )
    beside = crossed(own, 1)
    column = jnp.concatenate(
        [own[:256], beside[:256], crossed(other, 2), crossed(other, 3), own[256:], beside[256:]]
    )
    kv = [column] + [shifted(column, k) for k in (1, 2, 3)]

    all_lengths = arrived[:, 0, STATS + 6 * GROUP].astype(jnp.int32)
    live_of = jnp.clip((all_lengths - p + CLASSES - 1) // CLASSES, 0, class_rows)
    every_sample = jnp.arange(16)
    first = (jnp.arange(8)[None, :] - every_sample[:, None]) % 8
    held = jnp.clip((live_of[:, None] - first + 7) // 8, 0, 4)
    earlier = (every_sample[None, :] < every_sample[:, None])[:, :, None]
    before = jnp.sum(jnp.where(earlier, held[None], 0), axis=1)
    total = jnp.sum(held, axis=0)
    base = jnp.sum(jnp.where(jnp.arange(8)[None, :] < jnp.arange(8)[:, None], total[None], 0), axis=1)
    compact = call(
        compact_kernel,
        jax.ShapeDtypeStruct((8, 2 * SLOTS, 1024), BF16),
        p[None],
        z[None],
        arrived,
        in_specs=[smem, smem, vmem],
    )
    rows = exchange(compact, "sample_0")
    step = jnp.arange(SLOTS)[None, :]
    in_slot = base[:, None] + step
    in_slot = in_slot[:, None, :] + LIVE * jnp.arange(2)[None, :, None]
    in_slot = jnp.where((step < total[:, None])[:, None, :], in_slot, -1).reshape(1, 16 * SLOTS)
    k = jnp.arange(class_rows)
    holder = (k[None, :] + every_sample[:, None]) % 8
    chosen = holder[:, :, None] == jnp.arange(8)[None, None, :]
    slot_of = jnp.sum(jnp.where(chosen, (base[None, :] + before)[:, None, :], 0), axis=2)
    slot_of = jnp.where(k[None, :] < live_of[:, None], slot_of + k[None, :] // 8, -LIVE * 2)
    out_slot = slot_of.reshape(16, spans, 1, 4) + LIVE * jnp.arange(2)[None, None, :, None]
    out_slot = out_slot.reshape(1, 1024)

    live_rows = lax.broadcasted_iota(jnp.int32, (slice_rows, 1), 0) < live
    g_live = jnp.where(live_rows, g, jnp.zeros((), BF16))
    delta = jnp.sum(
        (g_live.astype(F32) * o.astype(F32)).reshape(slice_rows, heads, HEAD_WIDTH), axis=-1
    ).T
    own_rows = slice_rows // spans
    col_norms = lax.dynamic_slice_in_dim(log_norms[0], p * own_rows, own_rows, 1).T
    col_delta = lax.dynamic_slice_in_dim(delta, p * own_rows, own_rows, 1).T
    rows, delta, col_norms, col_delta = lax.optimization_barrier(
        (rows, delta, col_norms, col_delta)
    )
    own_shape = jax.ShapeDtypeStruct((own_rows, 2 * HEAD_WIDTH), BF16)
    gk_self, gv_self, gq_self = call(
        self_kernel,
        [own_shape, own_shape, jax.ShapeDtypeStruct((own_rows, heads * HEAD_WIDTH), F32)],
        p[None],
        lengths,
        q,
        g,
        norms,
        delta,
        col_norms,
        col_delta,
        *kv,
        in_specs=[smem] * 2 + [vmem] * 10,
    )

    kv_grads, gq_parts = prompt_terms(in_slot, out_slot, rows, *kv)
    gq_parts = exchange(gq_parts, SAMPLE_SPAN)
    parts = [kv_grads[0]] + [shifted(kv_grads[k], -k) for k in (1, 2, 3)]
    *parts, gq_self = lax.optimization_barrier((*parts, gq_self))
    parts = call(x_sum_kernel, [packed(256)] * 4, *parts)
    parts = [parts[0]] + [crossed(parts[k], k) for k in (1, 2, 3)]
    prompt_shape = jax.ShapeDtypeStruct(prompt_key_rows.shape, BF16)
    gk_prompt, gv_prompt = call(
        y_sum_kernel,
        [prompt_shape, prompt_shape],
        half[None],
        *parts,
        in_specs=[smem] + [vmem] * 4,
    )
    grad_query = call(
        final_kernel,
        jax.ShapeDtypeStruct((own_rows, heads * HEAD_WIDTH), BF16),
        gq_parts,
        gq_self,
        scratch_shapes=[pltpu.VMEM((heads * own_rows, HEAD_WIDTH), F32)],
    )
    return grad_query[None], gk_prompt, gv_prompt, gk_self[None], gv_self[None]


def solution(mesh):
    split = Mesh(
        mesh.devices.reshape(8, 2, 4, 2, mesh.shape["kvhead"]), SAMPLE_SPAN + ("kvhead",)
    )
    placed = (
        P(SAMPLE, None, "kvhead"),
        P(SAMPLE, None, "kvhead"),
        P(SAMPLE, None, "kvhead"),
        P(SAMPLE, "kvhead", None),
        P(SAMPLE),
        P(SAMPLE_SPAN, "kvhead"),
        P(SAMPLE_SPAN, "kvhead"),
        P(SAMPLE, SPAN, "kvhead"),
        P(SAMPLE, SPAN, "kvhead"),
    )

    return jax.shard_map(
        shards,
        mesh=split,
        in_specs=placed,
        out_specs=(
            P(SAMPLE, SPAN, "kvhead"),
            P(SAMPLE_SPAN, "kvhead"),
            P(SAMPLE_SPAN, "kvhead"),
            P(SAMPLE, SPAN, "kvhead"),
            P(SAMPLE, SPAN, "kvhead"),
        ),
        check_vma=False,
    )
```

```python
import math

import jax
import jax.numpy as jnp
from jax import lax
from jax.experimental import pallas as pl
from jax.experimental.pallas import tpu as pltpu
from jax.sharding import Mesh
from jax.sharding import PartitionSpec as P

HEAD_WIDTH = 128
SAMPLE = ("sample_0", "sample_1")
SPAN = ("span_0", "span_1")
SAMPLE_SPAN = SAMPLE + SPAN
ALONG_X, ALONG_Y = "span_0", ("sample_1", "span_1")
GROUP = 7
CLASSES = 8
SLOTS = 24
LIVE = 144
STATS = GROUP * HEAD_WIDTH
INTERPRET = False
VMEM_BYTES = 24 * 1024 * 1024
BF16 = jnp.bfloat16
F32 = jnp.float32
SCALE = 1.0 / math.sqrt(HEAD_WIDTH)
EXACT = lax.Precision.HIGHEST


def exchange(tiles, axes):
    return lax.all_to_all(tiles, axes, split_axis=0, concat_axis=0, tiled=True)


def dot(a, b, ca, cb):
    return lax.dot_general(a, b, (((ca,), (cb,)), ((), ())), preferred_element_type=F32)


def call(body, out_shape, *args, small=True, **kw):
    params = pltpu.CompilerParams(vmem_limit_bytes=VMEM_BYTES if small else None)
    return pl.pallas_call(
        body, out_shape=out_shape, interpret=INTERPRET, compiler_params=params, **kw
    )(*args)


def stat_lanes(shape):
    lane = lax.broadcasted_iota(jnp.int32, shape, 1)
    group = jnp.zeros(shape, jnp.int32)
    for edge in range(GROUP, 6 * GROUP, GROUP):
        group = group + jnp.where(lane >= edge, 1, 0)
    piece = jnp.where(group >= 3, group - 3, group)
    return lane, lane - GROUP * group, piece


def pick_kernel(p_ref, turn_ref, live_ref, q_ref, o_ref, g_ref, norm_ref, out_ref):
    p, turn, live = p_ref[0], turn_ref[0], live_ref[0]
    row = lax.broadcasted_iota(jnp.int32, (64, 256), 0)
    i = lax.broadcasted_iota(jnp.int32, (64, 256), 1)
    hit = (i % 8 == p) & (i < live) & ((turn + i // 8) % 8 == row // 8) & (i // 64 == row % 4)
    pick_q = jnp.where(hit & (row % 8 < 4), 1.0, 0.0)
    pick_g = jnp.where(hit & (row % 8 >= 4), 1.0, 0.0).astype(BF16)
    lane, head_of, piece = stat_lanes((64, HEAD_WIDTH))
    pick_q_low = pick_q.astype(BF16)
    for half in range(2):
        lanes = slice(half * STATS, (half + 1) * STATS)
        both = dot(pick_q_low, q_ref[:, lanes], 1, 0) + dot(pick_g, g_ref[:, lanes], 1, 0)
        out_ref[:, half, :, 0:STATS] = both.reshape(8, 8, STATS).astype(BF16)
        product = dot(pick_q_low, o_ref[:, lanes], 1, 0) * dot(pick_q_low, g_ref[:, lanes], 1, 0)
        stat = jnp.zeros((64, HEAD_WIDTH), F32)
        for inner in range(GROUP):
            mine = head_of == inner
            part = product[:, inner * HEAD_WIDTH : (inner + 1) * HEAD_WIDTH]
            delta = jnp.sum(part, axis=1, keepdims=True)
            norm = norm_ref[half * GROUP + inner]
            norm = jnp.sum(pick_q * norm, axis=1, keepdims=True) * math.sqrt(HEAD_WIDTH)
            stat = jnp.where(mine & (lane < 3 * GROUP), norm, stat)
            stat = jnp.where(mine & (lane >= 3 * GROUP) & (lane < 6 * GROUP), delta, stat)
        high = stat.astype(BF16).astype(F32)
        middle = (stat - high).astype(BF16).astype(F32)
        low = stat - high - middle
        stat = jnp.where(piece == 0, high, jnp.where(piece == 1, middle, low))
        stat = jnp.where(lane == 6 * GROUP, live.astype(F32), stat)
        out_ref[:, half, :, STATS:] = stat.reshape(8, 8, HEAD_WIDTH).astype(BF16)


def compact_kernel(p_ref, z_ref, rows_ref, out_ref):
    rows = rows_ref[...].reshape(128, 1024)
    shape = (128, 128)
    row = lax.broadcasted_iota(jnp.int32, shape, 0)
    col = lax.broadcasted_iota(jnp.int32, shape, 1)
    length = rows[:, STATS + 6 * GROUP : STATS + 6 * GROUP + 1].astype(F32)
    length = jnp.broadcast_to(length, shape).astype(jnp.int32)
    count = (length - p_ref[0] + 7) >> 3
    valid = 8 * (row & 3) + ((z_ref[0] - (row >> 3)) & 7) < count
    earlier = jnp.where(((col >> 3) < (row >> 3)) & (((col >> 2) & 1) == 0), 1.0, 0.0)
    before = dot(earlier.astype(BF16), jnp.where(valid, 1.0, 0.0).astype(BF16), 1, 0)
    place = before.astype(jnp.int32) + (row & 3) + SLOTS * ((row >> 2) & 1)
    pick = jnp.where(valid & (place == col), 1.0, 0.0).astype(BF16)
    rows = dot(pick, rows, 0, 0)[0 : 2 * SLOTS].astype(BF16)
    for copy in range(out_ref.shape[0]):
        out_ref[copy] = rows


def prompt_kernel(in_slot_ref, out_slot_ref, rows_ref, *refs):
    kv_refs, kvg_refs = refs[0:4], refs[4:8]
    gq_ref, q_scr, g_scr, acc_ref, back_ref = refs[8:]
    acc_ref[...] = jnp.zeros_like(acc_ref)
    slot = in_slot_ref[0:1, :]
    hit = lax.broadcasted_iota(jnp.int32, (2 * LIVE, slot.shape[1]), 0) == slot
    pick = jnp.where(hit, 1.0, 0.0).astype(BF16)
    rows = dot(pick, rows_ref[...].reshape(slot.shape[1], -1), 1, 0).astype(BF16)
    lane, head_of, _ = stat_lanes((LIVE, HEAD_WIDTH))
    stats = rows[0:LIVE, STATS:]
    zero = jnp.zeros((), BF16)
    for head in range(GROUP):
        place = slice(head * LIVE, (head + 1) * LIVE)
        lanes = slice(head * HEAD_WIDTH, (head + 1) * HEAD_WIDTH)
        mine = head_of == head
        q_scr[place, 0:HEAD_WIDTH] = rows[0:LIVE, lanes]
        q_scr[place, HEAD_WIDTH:] = jnp.where(mine & (lane < 3 * GROUP), stats, zero)
        g_scr[place, 0:HEAD_WIDTH] = rows[LIVE:, lanes]
        g_scr[place, HEAD_WIDTH:] = jnp.where(
            mine & (lane >= 3 * GROUP) & (lane < 6 * GROUP), stats, zero
        )
    q_scr[GROUP * LIVE :, :] = jnp.zeros((1024 - GROUP * LIVE, 2 * HEAD_WIDTH), BF16)
    g_scr[GROUP * LIVE :, :] = jnp.zeros((1024 - GROUP * LIVE, 2 * HEAD_WIDTH), BF16)

    lane = lax.broadcasted_iota(jnp.int32, (256, HEAD_WIDTH), 1)
    minus = jnp.where(lane < 6 * GROUP, -1.0, 0.0).astype(BF16)

    def block(kv_ref, kvg_ref, pair):
        def piece(k):
            return pl.ds(pl.multiple_of(pair * 512 + k * 128, 128), 128)

        keys = jnp.concatenate([kv_ref[piece(0), :], kv_ref[piece(2), :]], axis=0)
        values = jnp.concatenate([kv_ref[piece(1), :], kv_ref[piece(3), :]], axis=0)
        wide_keys = jnp.concatenate([keys, minus], axis=1)
        wide_values = jnp.concatenate([values, minus], axis=1)
        gk = jnp.zeros(keys.shape, F32)
        gv = jnp.zeros(keys.shape, F32)
        for part in range(4):
            rows = slice(256 * part, 256 * part + 256)
            prob = jnp.exp(dot(wide_keys, q_scr[rows, :], 1, 1) * SCALE)
            sgrad = (prob * dot(wide_values, g_scr[rows, :], 1, 1)).astype(BF16)
            gv = gv + dot(prob.astype(BF16), g_scr[rows, 0:HEAD_WIDTH], 1, 0)
            gk = gk + dot(sgrad, q_scr[rows, 0:HEAD_WIDTH], 1, 0)
            acc_ref[rows, :] += dot(sgrad, keys, 0, 0)
        gk, gv = (gk * SCALE).astype(BF16), gv.astype(BF16)
        for k, part in enumerate((gk[0:128], gv[0:128], gk[128:256], gv[128:256])):
            kvg_ref[piece(k), :] = part

    for kv_ref, kvg_ref in zip(kv_refs, kvg_refs):
        lax.fori_loop(0, 2, lambda k, _: block(kv_ref, kvg_ref, k), None)

    back_ref[...] = jnp.zeros_like(back_ref)
    for head in range(GROUP):
        lanes = slice(head % 4 * HEAD_WIDTH, (head % 4 + 1) * HEAD_WIDTH)
        part = (acc_ref[head * LIVE : (head + 1) * LIVE, :] * SCALE).astype(BF16)
        back_ref[head // 4 * LIVE : (head // 4 + 1) * LIVE, lanes] = part
    slot = out_slot_ref[0:1, :]
    hit = lax.broadcasted_iota(jnp.int32, (2 * LIVE, slot.shape[1]), 0) == slot
    pick = jnp.where(hit, 1.0, 0.0).astype(BF16)
    gq_ref[...] = dot(pick, back_ref[...], 0, 0).reshape(gq_ref.shape).astype(BF16)


def prompt_terms(in_slot, out_slot, rows, *kv):
    *kv_grads, gq = call(
        prompt_kernel,
        [jax.ShapeDtypeStruct((1024, HEAD_WIDTH), BF16)] * 4
        + [jax.ShapeDtypeStruct((128, 8, 512), BF16)],
        in_slot,
        out_slot,
        rows,
        *kv,
        small=False,
        scratch_shapes=[
            pltpu.VMEM((1024, 2 * HEAD_WIDTH), BF16),
            pltpu.VMEM((1024, 2 * HEAD_WIDTH), BF16),
            pltpu.VMEM((1024, HEAD_WIDTH), F32),
            pltpu.VMEM((2 * LIVE, 512), BF16),
        ],
    )
    return kv_grads, gq


def final_kernel(parts_ref, own_ref, out_ref, sum_ref):
    for half in range(2):
        for p in range(CLASSES):
            total = parts_ref[half * 8 + p].astype(F32)
            for z in range(1, 8):
                total = total + parts_ref[z * 16 + half * 8 + p].astype(F32)
            for head in range(GROUP):
                rows = slice(head // 4 * 4, head // 4 * 4 + 4)
                part = total[rows, head % 4 * HEAD_WIDTH : (head % 4 + 1) * HEAD_WIDTH]
                first = (half * GROUP + head) * 32 + p
                sum_ref[pl.ds(first, 4, stride=8), :] = part
    for head in range(2 * GROUP):
        lanes = slice(head * HEAD_WIDTH, (head + 1) * HEAD_WIDTH)
        out_ref[:, lanes] = (sum_ref[head * 32 : head * 32 + 32, :] + own_ref[:, lanes]).astype(BF16)


def pack_kernel(info, pk_ref, pv_ref, sk_ref, sv_ref, own_ref, other_ref):
    half = info[0]
    low, high = slice(0, HEAD_WIDTH), slice(HEAD_WIDTH, 2 * HEAD_WIDTH)
    for k, ref in enumerate((pk_ref, pv_ref)):
        rows = slice(128 * k, 128 * k + 128)
        own_ref[rows, :] = jnp.where(half == 0, ref[:, low], ref[:, high])
        other_ref[rows, :] = jnp.where(half == 0, ref[:, high], ref[:, low])
    for k, (ref, lanes) in enumerate(((sk_ref, low), (sk_ref, high), (sv_ref, low), (sv_ref, high))):
        own_ref[256 + 32 * k : 288 + 32 * k, :] = ref[:, lanes]


def x_sum_kernel(a_ref, b_ref, c_ref, d_ref, *out_refs):
    for k, out_ref in enumerate(out_refs):
        rows = slice(256 * k, 256 * k + 256)
        total = a_ref[rows, :].astype(F32) + b_ref[rows, :].astype(F32)
        total = total + c_ref[rows, :].astype(F32) + d_ref[rows, :].astype(F32)
        out_ref[...] = total.astype(BF16)


def y_sum_kernel(info, a_ref, b_ref, c_ref, d_ref, k_ref, v_ref):
    half = info[0]
    own = a_ref[...].astype(F32) + b_ref[...].astype(F32)
    other = c_ref[...].astype(F32) + d_ref[...].astype(F32)
    low = jnp.where(half == 0, own, other).astype(BF16)
    high = jnp.where(half == 0, other, own).astype(BF16)
    for k, ref in enumerate((k_ref, v_ref)):
        ref[:, 0:HEAD_WIDTH] = low[128 * k : 128 * k + 128]
        ref[:, HEAD_WIDTH:] = high[128 * k : 128 * k + 128]


def shifted(value, by):
    return lax.ppermute(value, ALONG_X, [(k, (k + by) % 4) for k in range(4)])


def crossed(value, by):
    return lax.ppermute(value, ALONG_Y, [(k, k ^ by) for k in range(4)])


def self_kernel(
    p_ref, live_ref, q_ref, o_ref, g_ref, norm_ref, kv0_ref, kv1_ref, kv2_ref, kv3_ref,
    gk_ref, gv_ref, gq_ref,
):
    p, live = p_ref[0], live_ref[0]
    rows_total = q_ref.shape[0]
    i_row = lax.broadcasted_iota(jnp.int32, (32, rows_total), 1)
    j_row = lax.broadcasted_iota(jnp.int32, (32, rows_total), 0) + p * 32
    live_row = lax.broadcasted_iota(jnp.int32, (rows_total, HEAD_WIDTH), 0) < live
    live_own = lax.broadcasted_iota(jnp.int32, (32, HEAD_WIDTH), 0) + p * 32 < live
    zero = jnp.zeros((), BF16)
    ones = jnp.ones((8, HEAD_WIDTH), F32)
    own = pl.ds(pl.multiple_of(p * 32, 32), 32)
    diagonal = i_row == j_row
    kv_refs = (kv0_ref, kv1_ref, kv2_ref, kv3_ref)
    lane = lax.broadcasted_iota(jnp.int32, (1, rows_total), 1)
    block = lane // 32
    from_span = (p // 2 + 4 - block // 2) % 4 * 2 + (p % 2 + block % 2) % 2
    position = from_span * 32 + lane % 32
    for kv in range(2):
        key_lanes = slice(kv * HEAD_WIDTH, (kv + 1) * HEAD_WIDTH)

        def piece(ref, which, kind):
            first = 1024 + 128 * which + 32 * (2 * kind + kv)
            return ref[first : first + 32, :]

        keys, values = piece(kv0_ref, 0, 0), piece(kv0_ref, 0, 1)
        all_keys = jnp.concatenate([piece(r, w, 0) for r in kv_refs for w in range(2)], axis=0)
        all_values = jnp.concatenate([piece(r, w, 1) for r in kv_refs for w in range(2)], axis=0)
        gk = jnp.zeros((32, HEAD_WIDTH), F32)
        gv = jnp.zeros((32, HEAD_WIDTH), F32)
        for inner in range(GROUP):
            head = kv * GROUP + inner
            lanes = slice(head * HEAD_WIDTH, (head + 1) * HEAD_WIDTH)
            q = q_ref[:, lanes]
            g = jnp.where(live_row, g_ref[:, lanes], zero)
            product = g.astype(F32) * o_ref[:, lanes].astype(F32)
            delta = lax.dot_general(
                ones, product, (((1,), (1,)), ((), ())), precision=EXACT, preferred_element_type=F32
            )
            prob = jnp.exp(dot(keys, q, 1, 1) * SCALE - norm_ref[head])
            prob = jnp.where(j_row <= i_row, prob, 0.0)
            sgrad = prob * (dot(values, g, 1, 1) - delta[0:1, :])
            gv = gv + dot(prob.astype(BF16), g, 1, 0)
            gk = gk + dot(sgrad.astype(BF16), q, 1, 0)
            q_own, g_own = q_ref[own, lanes], g_ref[own, lanes]
            g_own = jnp.where(live_own, g_own, zero)
            product = g_own.astype(F32) * o_ref[own, lanes].astype(F32)
            delta_own = jnp.sum(product, axis=1, keepdims=True)
            norm_own = jnp.sum(jnp.where(diagonal, norm_ref[head], 0.0), axis=1, keepdims=True)
            prob = jnp.exp(dot(q_own, all_keys, 1, 1) * SCALE - norm_own)
            i_own = lax.broadcasted_iota(jnp.int32, prob.shape, 0) + p * 32
            prob = jnp.where(position <= i_own, prob, 0.0)
            sgrad = prob * (dot(g_own, all_values, 1, 1) - delta_own)
            gq_ref[:, lanes] = dot(sgrad.astype(BF16), all_keys, 1, 0) * SCALE
        gk_ref[:, key_lanes] = (gk * SCALE).astype(BF16)
        gv_ref[:, key_lanes] = gv.astype(BF16)


def shards(
    queries,
    outputs,
    grad_out,
    log_norms,
    lengths,
    prompt_key_rows,
    prompt_value_rows,
    slice_key_rows,
    slice_value_rows,
):
    z = lax.axis_index("sample_0")
    half = lax.axis_index("sample_1")
    p = lax.axis_index(SPAN)
    sample = 2 * z + half
    spans = lax.axis_size(SPAN)
    slice_rows = queries.shape[1]
    heads = queries.shape[2] // HEAD_WIDTH
    class_rows = slice_rows // CLASSES
    q, o, g = queries[0], outputs[0], grad_out[0]
    norms = log_norms.transpose(1, 0, 2)
    smem, vmem = pl.BlockSpec(memory_space=pltpu.SMEM), pl.BlockSpec(memory_space=pltpu.VMEM)

    picked = call(
        pick_kernel,
        jax.ShapeDtypeStruct((8, 2, 8, 1024), BF16),
        p[None],
        (sample % 8)[None],
        lengths,
        q,
        o,
        g,
        norms,
        in_specs=[smem] * 3 + [vmem] * 4,
        small=False,
    )
    arrived = exchange(picked.reshape(16, 8, 1024), SAMPLE)

    packed = lambda rows: jax.ShapeDtypeStruct((rows, HEAD_WIDTH), BF16)
    own, other = call(
        pack_kernel,
        [packed(384), packed(256)],
        half[None],
        prompt_key_rows,
        prompt_value_rows,
        slice_key_rows[0],
        slice_value_rows[0],
        in_specs=[smem] + [vmem] * 4,
    )
    beside = crossed(own, 1)
    column = jnp.concatenate(
        [own[:256], beside[:256], crossed(other, 2), crossed(other, 3), own[256:], beside[256:]]
    )
    kv = [column] + [shifted(column, k) for k in (1, 2, 3)]

    all_lengths = arrived[:, 0, STATS + 6 * GROUP].astype(jnp.int32)
    live_of = jnp.clip((all_lengths - p + CLASSES - 1) // CLASSES, 0, class_rows)
    every_sample = jnp.arange(16)
    first = (jnp.arange(8)[None, :] - every_sample[:, None]) % 8
    held = jnp.clip((live_of[:, None] - first + 7) // 8, 0, 4)
    earlier = (every_sample[None, :] < every_sample[:, None])[:, :, None]
    before = jnp.sum(jnp.where(earlier, held[None], 0), axis=1)
    total = jnp.sum(held, axis=0)
    base = jnp.sum(jnp.where(jnp.arange(8)[None, :] < jnp.arange(8)[:, None], total[None], 0), axis=1)
    compact = call(
        compact_kernel,
        jax.ShapeDtypeStruct((8, 2 * SLOTS, 1024), BF16),
        p[None],
        z[None],
        arrived,
        in_specs=[smem, smem, vmem],
    )
    rows = exchange(compact, "sample_0")
    step = jnp.arange(SLOTS)[None, :]
    in_slot = base[:, None] + step
    in_slot = in_slot[:, None, :] + LIVE * jnp.arange(2)[None, :, None]
    in_slot = jnp.where((step < total[:, None])[:, None, :], in_slot, -1).reshape(1, 16 * SLOTS)
    k = jnp.arange(class_rows)
    holder = (k[None, :] + every_sample[:, None]) % 8
    chosen = holder[:, :, None] == jnp.arange(8)[None, None, :]
    slot_of = jnp.sum(jnp.where(chosen, (base[None, :] + before)[:, None, :], 0), axis=2)
    slot_of = jnp.where(k[None, :] < live_of[:, None], slot_of + k[None, :] // 8, -LIVE * 2)
    out_slot = slot_of.reshape(16, spans, 1, 4) + LIVE * jnp.arange(2)[None, None, :, None]
    out_slot = out_slot.reshape(1, 1024)

    own_rows = slice_rows // spans
    own_shape = jax.ShapeDtypeStruct((own_rows, 2 * HEAD_WIDTH), BF16)
    gk_self, gv_self, gq_self = call(
        self_kernel,
        [own_shape, own_shape, jax.ShapeDtypeStruct((own_rows, heads * HEAD_WIDTH), F32)],
        p[None],
        lengths,
        q,
        o,
        g,
        norms,
        *kv,
        in_specs=[smem] * 2 + [vmem] * 8,
        small=False,
    )

    kv_grads, gq_parts = prompt_terms(in_slot, out_slot, rows, *kv)
    parts = [kv_grads[0]] + [shifted(kv_grads[k], -k) for k in (1, 2, 3)]
    gq_parts = exchange(gq_parts, SAMPLE_SPAN)
    *parts, gq_self = lax.optimization_barrier((*parts, gq_self))
    parts = call(x_sum_kernel, [packed(256)] * 4, *parts)
    parts = [parts[0]] + [crossed(parts[k], k) for k in (1, 2, 3)]
    prompt_shape = jax.ShapeDtypeStruct(prompt_key_rows.shape, BF16)
    gk_prompt, gv_prompt = call(
        y_sum_kernel,
        [prompt_shape, prompt_shape],
        half[None],
        *parts,
        in_specs=[smem] + [vmem] * 4,
    )
    grad_query = call(
        final_kernel,
        jax.ShapeDtypeStruct((own_rows, heads * HEAD_WIDTH), BF16),
        gq_parts,
        gq_self,
        scratch_shapes=[pltpu.VMEM((heads * own_rows, HEAD_WIDTH), F32)],
    )
    return grad_query[None], gk_prompt, gv_prompt, gk_self[None], gv_self[None]


def solution(mesh):
    split = Mesh(
        mesh.devices.reshape(8, 2, 4, 2, mesh.shape["kvhead"]), SAMPLE_SPAN + ("kvhead",)
    )
    placed = (
        P(SAMPLE, None, "kvhead"),
        P(SAMPLE, None, "kvhead"),
        P(SAMPLE, None, "kvhead"),
        P(SAMPLE, "kvhead", None),
        P(SAMPLE),
        P(SAMPLE_SPAN, "kvhead"),
        P(SAMPLE_SPAN, "kvhead"),
        P(SAMPLE, SPAN, "kvhead"),
        P(SAMPLE, SPAN, "kvhead"),
    )

    return jax.shard_map(
        shards,
        mesh=split,
        in_specs=placed,
        out_specs=(
            P(SAMPLE, SPAN, "kvhead"),
            P(SAMPLE_SPAN, "kvhead"),
            P(SAMPLE_SPAN, "kvhead"),
            P(SAMPLE, SPAN, "kvhead"),
            P(SAMPLE, SPAN, "kvhead"),
        ),
        check_vma=False,
    )
```

```python
import math

import jax
import jax.numpy as jnp
from jax import lax
from jax.experimental import pallas as pl
from jax.experimental.pallas import tpu as pltpu
from jax.sharding import Mesh
from jax.sharding import PartitionSpec as P

HEAD_WIDTH = 128
SAMPLE = ("sample_0", "sample_1")
SPAN = ("span_0", "span_1")
SAMPLE_SPAN = SAMPLE + SPAN
ALONG_X, ALONG_Y = "span_0", ("sample_1", "span_1")
GROUP = 7
CLASSES = 8
SLOTS = 24
LIVE = 144
STATS = GROUP * HEAD_WIDTH
INTERPRET = False
KEY_BLOCK, ROW_BLOCK = 512, 512
VMEM_BYTES = 24 * 1024 * 1024
BF16 = jnp.bfloat16
F32 = jnp.float32
SCALE = 1.0 / math.sqrt(HEAD_WIDTH)
EXACT = lax.Precision.HIGHEST


def exchange(tiles, axes):
    return lax.all_to_all(tiles, axes, split_axis=0, concat_axis=0, tiled=True)


def dot(a, b, ca, cb):
    return lax.dot_general(a, b, (((ca,), (cb,)), ((), ())), preferred_element_type=F32)


def call(body, out_shape, *args, small=True, **kw):
    params = pltpu.CompilerParams(vmem_limit_bytes=VMEM_BYTES if small else None)
    return pl.pallas_call(
        body, out_shape=out_shape, interpret=INTERPRET, compiler_params=params, **kw
    )(*args)


def stat_lanes(shape):
    lane = lax.broadcasted_iota(jnp.int32, shape, 1)
    group = jnp.zeros(shape, jnp.int32)
    for edge in range(GROUP, 6 * GROUP, GROUP):
        group = group + jnp.where(lane >= edge, 1, 0)
    piece = jnp.where(group >= 3, group - 3, group)
    return lane, lane - GROUP * group, piece


def pick_kernel(p_ref, turn_ref, live_ref, q_ref, o_ref, g_ref, norm_ref, out_ref):
    p, turn, live = p_ref[0], turn_ref[0], live_ref[0]
    row = lax.broadcasted_iota(jnp.int32, (64, 256), 0)
    i = lax.broadcasted_iota(jnp.int32, (64, 256), 1)
    hit = (i % 8 == p) & (i < live) & ((turn + i // 8) % 8 == row // 8) & (i // 64 == row % 4)
    pick_q = jnp.where(hit & (row % 8 < 4), 1.0, 0.0)
    pick_g = jnp.where(hit & (row % 8 >= 4), 1.0, 0.0).astype(BF16)
    lane, head_of, piece = stat_lanes((64, HEAD_WIDTH))
    pick_q_low = pick_q.astype(BF16)
    for half in range(2):
        lanes = slice(half * STATS, (half + 1) * STATS)
        both = dot(pick_q_low, q_ref[:, lanes], 1, 0) + dot(pick_g, g_ref[:, lanes], 1, 0)
        out_ref[:, half, :, 0:STATS] = both.reshape(8, 8, STATS).astype(BF16)
        product = dot(pick_q_low, o_ref[:, lanes], 1, 0) * dot(pick_q_low, g_ref[:, lanes], 1, 0)
        stat = jnp.zeros((64, HEAD_WIDTH), F32)
        for inner in range(GROUP):
            mine = head_of == inner
            part = product[:, inner * HEAD_WIDTH : (inner + 1) * HEAD_WIDTH]
            delta = jnp.sum(part, axis=1, keepdims=True)
            norm = norm_ref[half * GROUP + inner]
            norm = jnp.sum(pick_q * norm, axis=1, keepdims=True) * math.sqrt(HEAD_WIDTH)
            stat = jnp.where(mine & (lane < 3 * GROUP), norm, stat)
            stat = jnp.where(mine & (lane >= 3 * GROUP) & (lane < 6 * GROUP), delta, stat)
        high = stat.astype(BF16).astype(F32)
        middle = (stat - high).astype(BF16).astype(F32)
        low = stat - high - middle
        stat = jnp.where(piece == 0, high, jnp.where(piece == 1, middle, low))
        stat = jnp.where(lane == 6 * GROUP, live.astype(F32), stat)
        out_ref[:, half, :, STATS:] = stat.reshape(8, 8, HEAD_WIDTH).astype(BF16)


def compact_kernel(p_ref, z_ref, rows_ref, out_ref):
    rows = rows_ref[...].reshape(128, 1024)
    shape = (128, 128)
    row = lax.broadcasted_iota(jnp.int32, shape, 0)
    col = lax.broadcasted_iota(jnp.int32, shape, 1)
    length = rows[:, STATS + 6 * GROUP : STATS + 6 * GROUP + 1].astype(F32)
    length = jnp.broadcast_to(length, shape).astype(jnp.int32)
    count = (length - p_ref[0] + 7) >> 3
    valid = 8 * (row & 3) + ((z_ref[0] - (row >> 3)) & 7) < count
    earlier = jnp.where(((col >> 3) < (row >> 3)) & (((col >> 2) & 1) == 0), 1.0, 0.0)
    before = dot(earlier.astype(BF16), jnp.where(valid, 1.0, 0.0).astype(BF16), 1, 0)
    place = before.astype(jnp.int32) + (row & 3) + SLOTS * ((row >> 2) & 1)
    pick = jnp.where(valid & (place == col), 1.0, 0.0).astype(BF16)
    rows = dot(pick, rows, 0, 0)[0 : 2 * SLOTS].astype(BF16)
    for copy in range(out_ref.shape[0]):
        out_ref[copy] = rows


def prompt_kernel(in_slot_ref, out_slot_ref, rows_ref, *refs):
    kv_refs, kvg_refs = refs[0:4], refs[4:8]
    gq_ref, q_scr, g_scr, acc_ref, back_ref = refs[8:]
    acc_ref[...] = jnp.zeros_like(acc_ref)
    slot = in_slot_ref[0:1, :]
    hit = lax.broadcasted_iota(jnp.int32, (2 * LIVE, slot.shape[1]), 0) == slot
    pick = jnp.where(hit, 1.0, 0.0).astype(BF16)
    rows = dot(pick, rows_ref[...].reshape(slot.shape[1], -1), 1, 0).astype(BF16)
    lane, head_of, _ = stat_lanes((LIVE, HEAD_WIDTH))
    stats = rows[0:LIVE, STATS:]
    zero = jnp.zeros((), BF16)
    for head in range(GROUP):
        place = slice(head * LIVE, (head + 1) * LIVE)
        lanes = slice(head * HEAD_WIDTH, (head + 1) * HEAD_WIDTH)
        mine = head_of == head
        q_scr[place, 0:HEAD_WIDTH] = rows[0:LIVE, lanes]
        q_scr[place, HEAD_WIDTH:] = jnp.where(mine & (lane < 3 * GROUP), stats, zero)
        g_scr[place, 0:HEAD_WIDTH] = rows[LIVE:, lanes]
        g_scr[place, HEAD_WIDTH:] = jnp.where(
            mine & (lane >= 3 * GROUP) & (lane < 6 * GROUP), stats, zero
        )
    q_scr[GROUP * LIVE :, :] = jnp.zeros((1024 - GROUP * LIVE, 2 * HEAD_WIDTH), BF16)
    g_scr[GROUP * LIVE :, :] = jnp.zeros((1024 - GROUP * LIVE, 2 * HEAD_WIDTH), BF16)

    lane = lax.broadcasted_iota(jnp.int32, (KEY_BLOCK, HEAD_WIDTH), 1)
    minus = jnp.where(lane < 6 * GROUP, -1.0, 0.0).astype(BF16)
    for kv_ref, kvg_ref in zip(kv_refs, kvg_refs):
        for first in range(0, 1024, 2 * KEY_BLOCK):
            starts = range(first, first + 2 * KEY_BLOCK, 256)
            keys = jnp.concatenate([kv_ref[k : k + 128, :] for k in starts], axis=0)
            values = jnp.concatenate([kv_ref[k + 128 : k + 256, :] for k in starts], axis=0)
            turned = keys.T
            wide_keys = jnp.concatenate([keys, minus], axis=1)
            wide_values = jnp.concatenate([values, minus], axis=1)
            gk = jnp.zeros(keys.shape, F32)
            gv = jnp.zeros(keys.shape, F32)
            for part in range(0, 1024, ROW_BLOCK):
                rows = slice(part, part + ROW_BLOCK)
                prob = jnp.exp2(dot(wide_keys, q_scr[rows, :], 1, 1) * (SCALE / math.log(2)))
                sgrad = (prob * dot(wide_values, g_scr[rows, :], 1, 1)).astype(BF16)
                gv = gv + dot(prob.astype(BF16), g_scr[rows, 0:HEAD_WIDTH], 1, 0)
                gk = gk + dot(sgrad, q_scr[rows, 0:HEAD_WIDTH], 1, 0)
                acc_ref[:, rows] += dot(turned, sgrad, 1, 0)
            for n, k in enumerate(starts):
                kvg_ref[k : k + 128, :] = (gk[128 * n : 128 * n + 128] * SCALE).astype(BF16)
                kvg_ref[k + 128 : k + 256, :] = gv[128 * n : 128 * n + 128].astype(BF16)

    back_ref[...] = jnp.zeros_like(back_ref)
    sums = acc_ref[...].T
    for head in range(GROUP):
        lanes = slice(head % 4 * HEAD_WIDTH, (head % 4 + 1) * HEAD_WIDTH)
        part = (sums[head * LIVE : (head + 1) * LIVE, :] * SCALE).astype(BF16)
        back_ref[head // 4 * LIVE : (head // 4 + 1) * LIVE, lanes] = part
    slot = out_slot_ref[0:1, :]
    hit = lax.broadcasted_iota(jnp.int32, (2 * LIVE, slot.shape[1]), 0) == slot
    pick = jnp.where(hit, 1.0, 0.0).astype(BF16)
    gq_ref[...] = dot(pick, back_ref[...], 0, 0).reshape(gq_ref.shape).astype(BF16)


def prompt_terms(in_slot, out_slot, rows, *kv):
    *kv_grads, gq = call(
        prompt_kernel,
        [pltpu.HBM((1024, HEAD_WIDTH), BF16)] * 4 + [pltpu.HBM((128, 8, 512), BF16)],
        in_slot,
        out_slot,
        rows,
        *kv,
        out_specs=[pl.BlockSpec(memory_space=pltpu.VMEM)] * 5,
        scratch_shapes=[
            pltpu.VMEM((1024, 2 * HEAD_WIDTH), BF16),
            pltpu.VMEM((1024, 2 * HEAD_WIDTH), BF16),
            pltpu.VMEM((HEAD_WIDTH, 1024), F32),
            pltpu.VMEM((2 * LIVE, 512), BF16),
        ],
    )
    return kv_grads, gq


def final_kernel(parts_ref, own_ref, out_ref, sum_ref):
    for half in range(2):
        for p in range(CLASSES):
            total = parts_ref[half * 8 + p].astype(F32)
            for z in range(1, 8):
                total = total + parts_ref[z * 16 + half * 8 + p].astype(F32)
            for head in range(GROUP):
                rows = slice(head // 4 * 4, head // 4 * 4 + 4)
                part = total[rows, head % 4 * HEAD_WIDTH : (head % 4 + 1) * HEAD_WIDTH]
                first = (half * GROUP + head) * 32 + p
                sum_ref[pl.ds(first, 4, stride=8), :] = part
    for head in range(2 * GROUP):
        lanes = slice(head * HEAD_WIDTH, (head + 1) * HEAD_WIDTH)
        out_ref[:, lanes] = (sum_ref[head * 32 : head * 32 + 32, :] + own_ref[:, lanes]).astype(BF16)


def pack_kernel(info, pk_ref, pv_ref, sk_ref, sv_ref, own_ref, other_ref):
    half = info[0]
    low, high = slice(0, HEAD_WIDTH), slice(HEAD_WIDTH, 2 * HEAD_WIDTH)
    for k, ref in enumerate((pk_ref, pv_ref)):
        rows = slice(128 * k, 128 * k + 128)
        own_ref[rows, :] = jnp.where(half == 0, ref[:, low], ref[:, high])
        other_ref[rows, :] = jnp.where(half == 0, ref[:, high], ref[:, low])
    for k, (ref, lanes) in enumerate(((sk_ref, low), (sk_ref, high), (sv_ref, low), (sv_ref, high))):
        own_ref[256 + 32 * k : 288 + 32 * k, :] = ref[:, lanes]


def join_kernel(own_ref, beside_ref, third_ref, fourth_ref, out_ref):
    for k, ref in enumerate((own_ref, beside_ref, third_ref, fourth_ref)):
        out_ref[256 * k : 256 * k + 256, :] = ref[0:256, :]
    out_ref[1024:1152, :] = own_ref[256:384, :]
    out_ref[1152:1280, :] = beside_ref[256:384, :]


def x_sum_kernel(a_ref, b_ref, c_ref, d_ref, *out_refs):
    for k, out_ref in enumerate(out_refs):
        rows = slice(256 * k, 256 * k + 256)
        total = a_ref[rows, :].astype(F32) + b_ref[rows, :].astype(F32)
        total = total + c_ref[rows, :].astype(F32) + d_ref[rows, :].astype(F32)
        out_ref[...] = total.astype(BF16)


def y_sum_kernel(info, a_ref, b_ref, c_ref, d_ref, k_ref, v_ref):
    half = info[0]
    own = a_ref[...].astype(F32) + b_ref[...].astype(F32)
    other = c_ref[...].astype(F32) + d_ref[...].astype(F32)
    low = jnp.where(half == 0, own, other).astype(BF16)
    high = jnp.where(half == 0, other, own).astype(BF16)
    for k, ref in enumerate((k_ref, v_ref)):
        ref[:, 0:HEAD_WIDTH] = low[128 * k : 128 * k + 128]
        ref[:, HEAD_WIDTH:] = high[128 * k : 128 * k + 128]


def shifted(value, by):
    return lax.ppermute(value, ALONG_X, [(k, (k + by) % 4) for k in range(4)])


def crossed(value, by):
    return lax.ppermute(value, ALONG_Y, [(k, k ^ by) for k in range(4)])


def self_kernel(
    p_ref, live_ref, q_ref, o_ref, g_ref, norm_ref, kv0_ref, kv1_ref, kv2_ref, kv3_ref,
    gk_ref, gv_ref, gq_ref,
):
    p, live = p_ref[0], live_ref[0]
    rows_total = q_ref.shape[0]
    i_row = lax.broadcasted_iota(jnp.int32, (32, rows_total), 1)
    j_row = lax.broadcasted_iota(jnp.int32, (32, rows_total), 0) + p * 32
    live_row = lax.broadcasted_iota(jnp.int32, (rows_total, HEAD_WIDTH), 0) < live
    live_own = lax.broadcasted_iota(jnp.int32, (32, HEAD_WIDTH), 0) + p * 32 < live
    zero = jnp.zeros((), BF16)
    ones = jnp.ones((8, HEAD_WIDTH), F32)
    own = pl.ds(pl.multiple_of(p * 32, 32), 32)
    diagonal = i_row == j_row
    kv_refs = (kv0_ref, kv1_ref, kv2_ref, kv3_ref)
    lane = lax.broadcasted_iota(jnp.int32, (1, rows_total), 1)
    block = lane // 32
    from_span = (p // 2 + 4 - block // 2) % 4 * 2 + (p % 2 + block % 2) % 2
    position = from_span * 32 + lane % 32
    for kv in range(2):
        key_lanes = slice(kv * HEAD_WIDTH, (kv + 1) * HEAD_WIDTH)

        def piece(ref, which, kind):
            first = 1024 + 128 * which + 32 * (2 * kind + kv)
            return ref[first : first + 32, :]

        keys, values = piece(kv0_ref, 0, 0), piece(kv0_ref, 0, 1)
        all_keys = jnp.concatenate([piece(r, w, 0) for r in kv_refs for w in range(2)], axis=0)
        all_values = jnp.concatenate([piece(r, w, 1) for r in kv_refs for w in range(2)], axis=0)
        gk = jnp.zeros((32, HEAD_WIDTH), F32)
        gv = jnp.zeros((32, HEAD_WIDTH), F32)
        for inner in range(GROUP):
            head = kv * GROUP + inner
            lanes = slice(head * HEAD_WIDTH, (head + 1) * HEAD_WIDTH)
            q = q_ref[:, lanes]
            g = jnp.where(live_row, g_ref[:, lanes], zero)
            product = g.astype(F32) * o_ref[:, lanes].astype(F32)
            delta = lax.dot_general(
                ones, product, (((1,), (1,)), ((), ())), precision=EXACT, preferred_element_type=F32
            )
            prob = jnp.exp(dot(keys, q, 1, 1) * SCALE - norm_ref[head])
            prob = jnp.where(j_row <= i_row, prob, 0.0)
            sgrad = prob * (dot(values, g, 1, 1) - delta[0:1, :])
            gv = gv + dot(prob.astype(BF16), g, 1, 0)
            gk = gk + dot(sgrad.astype(BF16), q, 1, 0)
            q_own, g_own = q_ref[own, lanes], g_ref[own, lanes]
            g_own = jnp.where(live_own, g_own, zero)
            product = g_own.astype(F32) * o_ref[own, lanes].astype(F32)
            delta_own = jnp.sum(product, axis=1, keepdims=True)
            norm_own = jnp.sum(jnp.where(diagonal, norm_ref[head], 0.0), axis=1, keepdims=True)
            prob = jnp.exp(dot(q_own, all_keys, 1, 1) * SCALE - norm_own)
            i_own = lax.broadcasted_iota(jnp.int32, prob.shape, 0) + p * 32
            prob = jnp.where(position <= i_own, prob, 0.0)
            sgrad = prob * (dot(g_own, all_values, 1, 1) - delta_own)
            gq_ref[:, lanes] = dot(sgrad.astype(BF16), all_keys, 1, 0) * SCALE
        gk_ref[:, key_lanes] = (gk * SCALE).astype(BF16)
        gv_ref[:, key_lanes] = gv.astype(BF16)


def shards(
    queries,
    outputs,
    grad_out,
    log_norms,
    lengths,
    prompt_key_rows,
    prompt_value_rows,
    slice_key_rows,
    slice_value_rows,
):
    z = lax.axis_index("sample_0")
    half = lax.axis_index("sample_1")
    p = lax.axis_index(SPAN)
    sample = 2 * z + half
    spans = lax.axis_size(SPAN)
    slice_rows = queries.shape[1]
    heads = queries.shape[2] // HEAD_WIDTH
    class_rows = slice_rows // CLASSES
    q, o, g = queries[0], outputs[0], grad_out[0]
    norms = log_norms.transpose(1, 0, 2)
    smem, vmem = pl.BlockSpec(memory_space=pltpu.SMEM), pl.BlockSpec(memory_space=pltpu.VMEM)

    picked = call(
        pick_kernel,
        jax.ShapeDtypeStruct((8, 2, 8, 1024), BF16),
        p[None],
        (sample % 8)[None],
        lengths,
        q,
        o,
        g,
        norms,
        in_specs=[smem] * 3 + [vmem] * 4,
        small=False,
    )
    arrived = exchange(picked.reshape(16, 8, 1024), SAMPLE)

    packed = lambda rows: jax.ShapeDtypeStruct((rows, HEAD_WIDTH), BF16)
    own, other = call(
        pack_kernel,
        [packed(384), packed(256)],
        half[None],
        prompt_key_rows,
        prompt_value_rows,
        slice_key_rows[0],
        slice_value_rows[0],
        in_specs=[smem] + [vmem] * 4,
    )
    around = [own, crossed(own, 1), crossed(other, 2), crossed(other, 3)]
    column = call(join_kernel, packed(1280), *around)
    kv = [column] + [shifted(column, k) for k in (1, 2, 3)]

    all_lengths = arrived[:, 0, STATS + 6 * GROUP].astype(jnp.int32)
    live_of = jnp.clip((all_lengths - p + CLASSES - 1) // CLASSES, 0, class_rows)
    every_sample = jnp.arange(16)
    first = (jnp.arange(8)[None, :] - every_sample[:, None]) % 8
    held = jnp.clip((live_of[:, None] - first + 7) // 8, 0, 4)
    earlier = (every_sample[None, :] < every_sample[:, None])[:, :, None]
    before = jnp.sum(jnp.where(earlier, held[None], 0), axis=1)
    total = jnp.sum(held, axis=0)
    base = jnp.sum(jnp.where(jnp.arange(8)[None, :] < jnp.arange(8)[:, None], total[None], 0), axis=1)
    compact = call(
        compact_kernel,
        jax.ShapeDtypeStruct((8, 2 * SLOTS, 1024), BF16),
        p[None],
        z[None],
        arrived,
        in_specs=[smem, smem, vmem],
    )
    rows = exchange(compact, "sample_0")
    step = jnp.arange(SLOTS)[None, :]
    in_slot = base[:, None] + step
    in_slot = in_slot[:, None, :] + LIVE * jnp.arange(2)[None, :, None]
    in_slot = jnp.where((step < total[:, None])[:, None, :], in_slot, -1).reshape(1, 16 * SLOTS)
    k = jnp.arange(class_rows)
    holder = (k[None, :] + every_sample[:, None]) % 8
    chosen = holder[:, :, None] == jnp.arange(8)[None, None, :]
    slot_of = jnp.sum(jnp.where(chosen, (base[None, :] + before)[:, None, :], 0), axis=2)
    slot_of = jnp.where(k[None, :] < live_of[:, None], slot_of + k[None, :] // 8, -LIVE * 2)
    out_slot = slot_of.reshape(16, spans, 1, 4) + LIVE * jnp.arange(2)[None, None, :, None]
    out_slot = out_slot.reshape(1, 1024)

    own_rows = slice_rows // spans
    own_shape = jax.ShapeDtypeStruct((own_rows, 2 * HEAD_WIDTH), BF16)
    gk_self, gv_self, gq_self = call(
        self_kernel,
        [own_shape, own_shape, jax.ShapeDtypeStruct((own_rows, heads * HEAD_WIDTH), F32)],
        p[None],
        lengths,
        q,
        o,
        g,
        norms,
        *kv,
        in_specs=[smem] * 2 + [vmem] * 8,
        small=False,
    )

    kv_grads, gq_parts = prompt_terms(in_slot, out_slot, rows, *kv)
    parts = [kv_grads[0]] + [shifted(kv_grads[k], -k) for k in (1, 2, 3)]
    gq_parts = exchange(gq_parts, SAMPLE_SPAN)
    *parts, gq_self = lax.optimization_barrier((*parts, gq_self))
    parts = call(x_sum_kernel, [packed(256)] * 4, *parts)
    parts = [parts[0]] + [crossed(parts[k], k) for k in (1, 2, 3)]
    prompt_shape = jax.ShapeDtypeStruct(prompt_key_rows.shape, BF16)
    gk_prompt, gv_prompt = call(
        y_sum_kernel,
        [prompt_shape, prompt_shape],
        half[None],
        *parts,
        in_specs=[smem] + [vmem] * 4,
    )
    grad_query = call(
        final_kernel,
        jax.ShapeDtypeStruct((own_rows, heads * HEAD_WIDTH), BF16),
        gq_parts,
        gq_self,
        scratch_shapes=[pltpu.VMEM((heads * own_rows, HEAD_WIDTH), F32)],
    )
    return grad_query[None], gk_prompt, gv_prompt, gk_self[None], gv_self[None]


def solution(mesh):
    split = Mesh(
        mesh.devices.reshape(8, 2, 4, 2, mesh.shape["kvhead"]), SAMPLE_SPAN + ("kvhead",)
    )
    placed = (
        P(SAMPLE, None, "kvhead"),
        P(SAMPLE, None, "kvhead"),
        P(SAMPLE, None, "kvhead"),
        P(SAMPLE, "kvhead", None),
        P(SAMPLE),
        P(SAMPLE_SPAN, "kvhead"),
        P(SAMPLE_SPAN, "kvhead"),
        P(SAMPLE, SPAN, "kvhead"),
        P(SAMPLE, SPAN, "kvhead"),
    )

    return jax.shard_map(
        shards,
        mesh=split,
        in_specs=placed,
        out_specs=(
            P(SAMPLE, SPAN, "kvhead"),
            P(SAMPLE_SPAN, "kvhead"),
            P(SAMPLE_SPAN, "kvhead"),
            P(SAMPLE, SPAN, "kvhead"),
            P(SAMPLE, SPAN, "kvhead"),
        ),
        check_vma=False,
    )
```

```python
import math

import jax
import jax.numpy as jnp
from jax import lax
from jax.experimental import pallas as pl
from jax.experimental.pallas import tpu as pltpu
from jax.sharding import Mesh
from jax.sharding import PartitionSpec as P

HEAD_WIDTH = 128
SAMPLE = ("sample_0", "sample_1")
SPAN = ("span_0", "span_1")
SAMPLE_SPAN = SAMPLE + SPAN
ALONG_X, ALONG_Y = "span_0", ("sample_1", "span_1")
GROUP = 7
CLASSES = 8
SLOTS = 24
LIVE = 144
STATS = GROUP * HEAD_WIDTH
INTERPRET = False
KEY_BLOCK, ROW_BLOCK = 512, 512
VMEM_BYTES = 24 * 1024 * 1024
BF16 = jnp.bfloat16
F32 = jnp.float32
SCALE = 1.0 / math.sqrt(HEAD_WIDTH)
EXACT = lax.Precision.HIGHEST


def exchange(tiles, axes):
    return lax.all_to_all(tiles, axes, split_axis=0, concat_axis=0, tiled=True)


def dot(a, b, ca, cb):
    return lax.dot_general(a, b, (((ca,), (cb,)), ((), ())), preferred_element_type=F32)


def call(body, out_shape, *args, small=True, **kw):
    params = pltpu.CompilerParams(vmem_limit_bytes=VMEM_BYTES if small else None)
    return pl.pallas_call(
        body, out_shape=out_shape, interpret=INTERPRET, compiler_params=params, **kw
    )(*args)


def stat_lanes(shape):
    lane = lax.broadcasted_iota(jnp.int32, shape, 1)
    group = jnp.zeros(shape, jnp.int32)
    for edge in range(GROUP, 6 * GROUP, GROUP):
        group = group + jnp.where(lane >= edge, 1, 0)
    piece = jnp.where(group >= 3, group - 3, group)
    return lane, lane - GROUP * group, piece


def pick_kernel(p_ref, turn_ref, live_ref, q_ref, o_ref, g_ref, norm_ref, out_ref):
    p, turn, live = p_ref[0], turn_ref[0], live_ref[0]
    row = lax.broadcasted_iota(jnp.int32, (64, 256), 0)
    i = lax.broadcasted_iota(jnp.int32, (64, 256), 1)
    hit = (i % 8 == p) & (i < live) & ((turn + i // 8) % 8 == row // 8) & (i // 64 == row % 4)
    pick_q = jnp.where(hit & (row % 8 < 4), 1.0, 0.0)
    pick_g = jnp.where(hit & (row % 8 >= 4), 1.0, 0.0).astype(BF16)
    lane, head_of, piece = stat_lanes((64, HEAD_WIDTH))
    pick_q_low = pick_q.astype(BF16)
    both = dot(pick_q_low, q_ref[...], 1, 0) + dot(pick_g, g_ref[...], 1, 0)
    out_ref[:, 0, :, 0:STATS] = both.reshape(8, 8, STATS).astype(BF16)
    product = dot(pick_q_low, o_ref[...], 1, 0) * dot(pick_q_low, g_ref[...], 1, 0)
    stat = jnp.zeros((64, HEAD_WIDTH), F32)
    for inner in range(GROUP):
        mine = head_of == inner
        part = product[:, inner * HEAD_WIDTH : (inner + 1) * HEAD_WIDTH]
        delta = jnp.sum(part, axis=1, keepdims=True)
        norm = norm_ref[inner]
        norm = jnp.sum(pick_q * norm, axis=1, keepdims=True) * math.sqrt(HEAD_WIDTH)
        stat = jnp.where(mine & (lane < 3 * GROUP), norm, stat)
        stat = jnp.where(mine & (lane >= 3 * GROUP) & (lane < 6 * GROUP), delta, stat)
    high = stat.astype(BF16).astype(F32)
    middle = (stat - high).astype(BF16).astype(F32)
    low = stat - high - middle
    stat = jnp.where(piece == 0, high, jnp.where(piece == 1, middle, low))
    stat = jnp.where(lane == 6 * GROUP, live.astype(F32), stat)
    out_ref[:, 0, :, STATS:] = stat.reshape(8, 8, HEAD_WIDTH).astype(BF16)


def compact_kernel(p_ref, z_ref, rows_ref, out_ref):
    rows = rows_ref[...].reshape(128, 1024)
    shape = (128, 128)
    row = lax.broadcasted_iota(jnp.int32, shape, 0)
    col = lax.broadcasted_iota(jnp.int32, shape, 1)
    length = rows[:, STATS + 6 * GROUP : STATS + 6 * GROUP + 1].astype(F32)
    length = jnp.broadcast_to(length, shape).astype(jnp.int32)
    count = (length - p_ref[0] + 7) >> 3
    valid = 8 * (row & 3) + ((z_ref[0] - (row >> 3)) & 7) < count
    earlier = jnp.where(((col >> 3) < (row >> 3)) & (((col >> 2) & 1) == 0), 1.0, 0.0)
    before = dot(earlier.astype(BF16), jnp.where(valid, 1.0, 0.0).astype(BF16), 1, 0)
    place = before.astype(jnp.int32) + (row & 3) + SLOTS * ((row >> 2) & 1)
    pick = jnp.where(valid & (place == col), 1.0, 0.0).astype(BF16)
    rows = dot(pick, rows, 0, 0)[0 : 2 * SLOTS].astype(BF16)
    for copy in range(out_ref.shape[0]):
        out_ref[copy] = rows


def prompt_kernel(in_slot_ref, out_slot_ref, rows_ref, *refs):
    kv_refs, kvg_refs = refs[0:4], refs[4:8]
    gq_ref, q_scr, g_scr, acc_ref, back_ref = refs[8:]
    acc_ref[...] = jnp.zeros_like(acc_ref)
    slot = in_slot_ref[0:1, :]
    hit = lax.broadcasted_iota(jnp.int32, (2 * LIVE, slot.shape[1]), 0) == slot
    pick = jnp.where(hit, 1.0, 0.0).astype(BF16)
    rows = dot(pick, rows_ref[...].reshape(slot.shape[1], -1), 1, 0).astype(BF16)
    lane, head_of, _ = stat_lanes((LIVE, HEAD_WIDTH))
    stats = rows[0:LIVE, STATS:]
    zero = jnp.zeros((), BF16)
    for head in range(GROUP):
        place = slice(head * LIVE, (head + 1) * LIVE)
        lanes = slice(head * HEAD_WIDTH, (head + 1) * HEAD_WIDTH)
        mine = head_of == head
        q_scr[place, 0:HEAD_WIDTH] = rows[0:LIVE, lanes]
        q_scr[place, HEAD_WIDTH:] = jnp.where(mine & (lane < 3 * GROUP), stats, zero)
        g_scr[place, 0:HEAD_WIDTH] = rows[LIVE:, lanes]
        g_scr[place, HEAD_WIDTH:] = jnp.where(
            mine & (lane >= 3 * GROUP) & (lane < 6 * GROUP), stats, zero
        )
    q_scr[GROUP * LIVE :, :] = jnp.zeros((1024 - GROUP * LIVE, 2 * HEAD_WIDTH), BF16)
    g_scr[GROUP * LIVE :, :] = jnp.zeros((1024 - GROUP * LIVE, 2 * HEAD_WIDTH), BF16)

    lane = lax.broadcasted_iota(jnp.int32, (KEY_BLOCK, HEAD_WIDTH), 1)
    minus = jnp.where(lane < 6 * GROUP, -1.0, 0.0).astype(BF16)
    for kv_ref, kvg_ref in zip(kv_refs, kvg_refs):
        for first in range(0, 1024, 2 * KEY_BLOCK):
            starts = range(first, first + 2 * KEY_BLOCK, 256)
            keys = jnp.concatenate([kv_ref[k : k + 128, :] for k in starts], axis=0)
            values = jnp.concatenate([kv_ref[k + 128 : k + 256, :] for k in starts], axis=0)
            turned = keys.T
            wide_keys = jnp.concatenate([keys, minus], axis=1)
            wide_values = jnp.concatenate([values, minus], axis=1)
            gk = jnp.zeros(keys.shape, F32)
            gv = jnp.zeros(keys.shape, F32)
            for part in range(0, 1024, ROW_BLOCK):
                rows = slice(part, part + ROW_BLOCK)
                prob = jnp.exp2(dot(wide_keys, q_scr[rows, :], 1, 1) * (SCALE / math.log(2)))
                sgrad = (prob * dot(wide_values, g_scr[rows, :], 1, 1)).astype(BF16)
                gv = gv + dot(prob.astype(BF16), g_scr[rows, 0:HEAD_WIDTH], 1, 0)
                gk = gk + dot(sgrad, q_scr[rows, 0:HEAD_WIDTH], 1, 0)
                acc_ref[:, rows] += dot(turned, sgrad, 1, 0)
            for n, k in enumerate(starts):
                kvg_ref[k : k + 128, :] = (gk[128 * n : 128 * n + 128] * SCALE).astype(BF16)
                kvg_ref[k + 128 : k + 256, :] = gv[128 * n : 128 * n + 128].astype(BF16)

    back_ref[...] = jnp.zeros_like(back_ref)
    sums = acc_ref[...].T
    for head in range(GROUP):
        lanes = slice(head % 4 * HEAD_WIDTH, (head % 4 + 1) * HEAD_WIDTH)
        part = (sums[head * LIVE : (head + 1) * LIVE, :] * SCALE).astype(BF16)
        back_ref[head // 4 * LIVE : (head // 4 + 1) * LIVE, lanes] = part
    slot = out_slot_ref[0:1, :]
    hit = lax.broadcasted_iota(jnp.int32, (2 * LIVE, slot.shape[1]), 0) == slot
    pick = jnp.where(hit, 1.0, 0.0).astype(BF16)
    gq_ref[...] = dot(pick, back_ref[...], 0, 0).reshape(gq_ref.shape).astype(BF16)


def prompt_terms(in_slot, out_slot, rows, *kv):
    *kv_grads, gq = call(
        prompt_kernel,
        [pltpu.HBM((1024, HEAD_WIDTH), BF16)] * 4 + [pltpu.HBM((128, 8, 512), BF16)],
        in_slot,
        out_slot,
        rows,
        *kv,
        out_specs=[pl.BlockSpec(memory_space=pltpu.VMEM)] * 5,
        scratch_shapes=[
            pltpu.VMEM((1024, 2 * HEAD_WIDTH), BF16),
            pltpu.VMEM((1024, 2 * HEAD_WIDTH), BF16),
            pltpu.VMEM((HEAD_WIDTH, 1024), F32),
            pltpu.VMEM((2 * LIVE, 512), BF16),
        ],
    )
    return kv_grads, gq


def final_kernel(parts_ref, own_ref, out_ref, sum_ref):
    for half in range(2):
        for p in range(CLASSES):
            total = parts_ref[half * 8 + p].astype(F32)
            for z in range(1, 8):
                total = total + parts_ref[z * 16 + half * 8 + p].astype(F32)
            for head in range(GROUP):
                rows = slice(head // 4 * 4, head // 4 * 4 + 4)
                part = total[rows, head % 4 * HEAD_WIDTH : (head % 4 + 1) * HEAD_WIDTH]
                first = (half * GROUP + head) * 32 + p
                sum_ref[pl.ds(first, 4, stride=8), :] = part
    for head in range(2 * GROUP):
        lanes = slice(head * HEAD_WIDTH, (head + 1) * HEAD_WIDTH)
        out_ref[:, lanes] = (sum_ref[head * 32 : head * 32 + 32, :] + own_ref[:, lanes]).astype(BF16)


def pack_kernel(info, pk_ref, pv_ref, sk_ref, sv_ref, own_ref, other_ref):
    half = info[0]
    low, high = slice(0, HEAD_WIDTH), slice(HEAD_WIDTH, 2 * HEAD_WIDTH)
    for k, ref in enumerate((pk_ref, pv_ref)):
        rows = slice(128 * k, 128 * k + 128)
        own_ref[rows, :] = jnp.where(half == 0, ref[:, low], ref[:, high])
        other_ref[rows, :] = jnp.where(half == 0, ref[:, high], ref[:, low])
    for k, (ref, lanes) in enumerate(((sk_ref, low), (sk_ref, high), (sv_ref, low), (sv_ref, high))):
        own_ref[256 + 32 * k : 288 + 32 * k, :] = ref[:, lanes]


def join_kernel(own_ref, beside_ref, third_ref, fourth_ref, out_ref):
    for k, ref in enumerate((own_ref, beside_ref, third_ref, fourth_ref)):
        out_ref[256 * k : 256 * k + 256, :] = ref[0:256, :]
    out_ref[1024:1152, :] = own_ref[256:384, :]
    out_ref[1152:1280, :] = beside_ref[256:384, :]


def relay_kernel(own_ref, relayed_ref, out_ref):
    out_ref[...] = (own_ref[...].astype(F32) + relayed_ref[...].astype(F32)).astype(BF16)


def x_sum_kernel(a_ref, b_ref, c_ref, *out_refs):
    for k, out_ref in enumerate(out_refs):
        rows = slice(256 * k, 256 * k + 256)
        total = a_ref[rows, :].astype(F32) + b_ref[rows, :].astype(F32)
        out_ref[...] = (total + c_ref[rows, :].astype(F32)).astype(BF16)


def y_sum_kernel(info, a_ref, b_ref, c_ref, d_ref, k_ref, v_ref):
    half = info[0]
    own = a_ref[...].astype(F32) + b_ref[...].astype(F32)
    other = c_ref[...].astype(F32) + d_ref[...].astype(F32)
    low = jnp.where(half == 0, own, other).astype(BF16)
    high = jnp.where(half == 0, other, own).astype(BF16)
    for k, ref in enumerate((k_ref, v_ref)):
        ref[:, 0:HEAD_WIDTH] = low[128 * k : 128 * k + 128]
        ref[:, HEAD_WIDTH:] = high[128 * k : 128 * k + 128]


def shifted(value, by):
    return lax.ppermute(value, ALONG_X, [(k, (k + by) % 4) for k in range(4)])


def crossed(value, by):
    return lax.ppermute(value, ALONG_Y, [(k, k ^ by) for k in range(4)])


def self_kernel(
    p_ref, live_ref, q_ref, o_ref, g_ref, norm_ref, kv0_ref, kv1_ref, kv2_ref, kv3_ref,
    gk_ref, gv_ref, gq_ref,
):
    p, live = p_ref[0], live_ref[0]
    rows_total = q_ref.shape[0]
    i_row = lax.broadcasted_iota(jnp.int32, (32, rows_total), 1)
    j_row = lax.broadcasted_iota(jnp.int32, (32, rows_total), 0) + p * 32
    live_row = lax.broadcasted_iota(jnp.int32, (rows_total, HEAD_WIDTH), 0) < live
    live_own = lax.broadcasted_iota(jnp.int32, (32, HEAD_WIDTH), 0) + p * 32 < live
    zero = jnp.zeros((), BF16)
    ones = jnp.ones((8, HEAD_WIDTH), F32)
    own = pl.ds(pl.multiple_of(p * 32, 32), 32)
    diagonal = i_row == j_row
    kv_refs = (kv0_ref, kv1_ref, kv2_ref, kv3_ref)
    lane = lax.broadcasted_iota(jnp.int32, (1, rows_total), 1)
    block = lane // 32
    from_span = (p // 2 + 4 - block // 2) % 4 * 2 + (p % 2 + block % 2) % 2
    position = from_span * 32 + lane % 32
    for kv in range(2):
        key_lanes = slice(kv * HEAD_WIDTH, (kv + 1) * HEAD_WIDTH)

        def piece(ref, which, kind):
            first = 1024 + 128 * which + 32 * (2 * kind + kv)
            return ref[first : first + 32, :]

        keys, values = piece(kv0_ref, 0, 0), piece(kv0_ref, 0, 1)
        all_keys = jnp.concatenate([piece(r, w, 0) for r in kv_refs for w in range(2)], axis=0)
        all_values = jnp.concatenate([piece(r, w, 1) for r in kv_refs for w in range(2)], axis=0)
        gk = jnp.zeros((32, HEAD_WIDTH), F32)
        gv = jnp.zeros((32, HEAD_WIDTH), F32)
        for inner in range(GROUP):
            head = kv * GROUP + inner
            lanes = slice(head * HEAD_WIDTH, (head + 1) * HEAD_WIDTH)
            q = q_ref[:, lanes]
            g = jnp.where(live_row, g_ref[:, lanes], zero)
            product = g.astype(F32) * o_ref[:, lanes].astype(F32)
            delta = lax.dot_general(
                ones, product, (((1,), (1,)), ((), ())), precision=EXACT, preferred_element_type=F32
            )
            prob = jnp.exp(dot(keys, q, 1, 1) * SCALE - norm_ref[head])
            prob = jnp.where(j_row <= i_row, prob, 0.0)
            sgrad = prob * (dot(values, g, 1, 1) - delta[0:1, :])
            gv = gv + dot(prob.astype(BF16), g, 1, 0)
            gk = gk + dot(sgrad.astype(BF16), q, 1, 0)
            q_own, g_own = q_ref[own, lanes], g_ref[own, lanes]
            g_own = jnp.where(live_own, g_own, zero)
            product = g_own.astype(F32) * o_ref[own, lanes].astype(F32)
            delta_own = jnp.sum(product, axis=1, keepdims=True)
            norm_own = jnp.sum(jnp.where(diagonal, norm_ref[head], 0.0), axis=1, keepdims=True)
            prob = jnp.exp(dot(q_own, all_keys, 1, 1) * SCALE - norm_own)
            i_own = lax.broadcasted_iota(jnp.int32, prob.shape, 0) + p * 32
            prob = jnp.where(position <= i_own, prob, 0.0)
            sgrad = prob * (dot(g_own, all_values, 1, 1) - delta_own)
            gq_ref[:, lanes] = dot(sgrad.astype(BF16), all_keys, 1, 0) * SCALE
        gk_ref[:, key_lanes] = (gk * SCALE).astype(BF16)
        gv_ref[:, key_lanes] = gv.astype(BF16)


def shards(
    queries,
    outputs,
    grad_out,
    log_norms,
    lengths,
    prompt_key_rows,
    prompt_value_rows,
    slice_key_rows,
    slice_value_rows,
):
    z = lax.axis_index("sample_0")
    half = lax.axis_index("sample_1")
    p = lax.axis_index(SPAN)
    sample = 2 * z + half
    spans = lax.axis_size(SPAN)
    slice_rows = queries.shape[1]
    heads = queries.shape[2] // HEAD_WIDTH
    class_rows = slice_rows // CLASSES
    q, o, g = queries[0], outputs[0], grad_out[0]
    norms = log_norms.transpose(1, 0, 2)
    smem, vmem = pl.BlockSpec(memory_space=pltpu.SMEM), pl.BlockSpec(memory_space=pltpu.VMEM)

    picked = call(
        pick_kernel,
        jax.ShapeDtypeStruct((8, 2, 8, 1024), BF16),
        p[None],
        (sample % 8)[None],
        lengths,
        q,
        o,
        g,
        norms,
        grid=(2,),
        in_specs=[smem] * 3
        + [pl.BlockSpec((slice_rows, STATS), lambda k: (0, k))] * 3
        + [pl.BlockSpec((GROUP, 1, slice_rows), lambda k: (k, 0, 0))],
        out_specs=pl.BlockSpec((8, 1, 8, 1024), lambda k: (0, k, 0, 0)),
        small=False,
    )
    arrived = exchange(picked.reshape(16, 8, 1024), SAMPLE)

    packed = lambda rows: jax.ShapeDtypeStruct((rows, HEAD_WIDTH), BF16)
    own, other = call(
        pack_kernel,
        [packed(384), packed(256)],
        half[None],
        prompt_key_rows,
        prompt_value_rows,
        slice_key_rows[0],
        slice_value_rows[0],
        in_specs=[smem] + [vmem] * 4,
    )
    around = [own, crossed(own, 1), crossed(other, 2), crossed(other, 3)]
    column = call(join_kernel, packed(1280), *around)
    kv = [column] + [shifted(column, k) for k in (1, 2, 3)]

    all_lengths = arrived[:, 0, STATS + 6 * GROUP].astype(jnp.int32)
    live_of = jnp.clip((all_lengths - p + CLASSES - 1) // CLASSES, 0, class_rows)
    every_sample = jnp.arange(16)
    first = (jnp.arange(8)[None, :] - every_sample[:, None]) % 8
    held = jnp.clip((live_of[:, None] - first + 7) // 8, 0, 4)
    earlier = (every_sample[None, :] < every_sample[:, None])[:, :, None]
    before = jnp.sum(jnp.where(earlier, held[None], 0), axis=1)
    total = jnp.sum(held, axis=0)
    base = jnp.sum(jnp.where(jnp.arange(8)[None, :] < jnp.arange(8)[:, None], total[None], 0), axis=1)
    compact = call(
        compact_kernel,
        jax.ShapeDtypeStruct((8, 2 * SLOTS, 1024), BF16),
        p[None],
        z[None],
        arrived,
        in_specs=[smem, smem, vmem],
    )
    rows = exchange(compact, "sample_0")
    step = jnp.arange(SLOTS)[None, :]
    in_slot = base[:, None] + step
    in_slot = in_slot[:, None, :] + LIVE * jnp.arange(2)[None, :, None]
    in_slot = jnp.where((step < total[:, None])[:, None, :], in_slot, -1).reshape(1, 16 * SLOTS)
    k = jnp.arange(class_rows)
    holder = (k[None, :] + every_sample[:, None]) % 8
    chosen = holder[:, :, None] == jnp.arange(8)[None, None, :]
    slot_of = jnp.sum(jnp.where(chosen, (base[None, :] + before)[:, None, :], 0), axis=2)
    slot_of = jnp.where(k[None, :] < live_of[:, None], slot_of + k[None, :] // 8, -LIVE * 2)
    out_slot = slot_of.reshape(16, spans, 1, 4) + LIVE * jnp.arange(2)[None, None, :, None]
    out_slot = out_slot.reshape(1, 1024)

    kv_grads, gq_parts = prompt_terms(in_slot, out_slot, rows, *kv)
    relayed = shifted(kv_grads[2], -1)
    ahead = shifted(kv_grads[3], 1)
    gq_parts = exchange(gq_parts, SAMPLE_SPAN)
    joined = call(relay_kernel, packed(1024), kv_grads[1], relayed)
    behind = shifted(joined, -1)
    own_rows = slice_rows // spans
    own_shape = jax.ShapeDtypeStruct((own_rows, 2 * HEAD_WIDTH), BF16)
    gk_self, gv_self, gq_self = call(
        self_kernel,
        [own_shape, own_shape, jax.ShapeDtypeStruct((own_rows, heads * HEAD_WIDTH), F32)],
        p[None],
        lengths,
        q,
        o,
        g,
        norms,
        *kv,
        in_specs=[smem] * 2 + [vmem] * 8,
        small=False,
    )
    parts = call(x_sum_kernel, [packed(256)] * 4, kv_grads[0], ahead, behind)
    parts = [parts[0]] + [crossed(parts[k], k) for k in (1, 2, 3)]
    prompt_shape = jax.ShapeDtypeStruct(prompt_key_rows.shape, BF16)
    gk_prompt, gv_prompt = call(
        y_sum_kernel,
        [prompt_shape, prompt_shape],
        half[None],
        *parts,
        in_specs=[smem] + [vmem] * 4,
    )
    grad_query = call(
        final_kernel,
        jax.ShapeDtypeStruct((own_rows, heads * HEAD_WIDTH), BF16),
        gq_parts,
        gq_self,
        scratch_shapes=[pltpu.VMEM((heads * own_rows, HEAD_WIDTH), F32)],
    )
    return grad_query[None], gk_prompt, gv_prompt, gk_self[None], gv_self[None]


def solution(mesh):
    split = Mesh(
        mesh.devices.reshape(8, 2, 4, 2, mesh.shape["kvhead"]), SAMPLE_SPAN + ("kvhead",)
    )
    placed = (
        P(SAMPLE, None, "kvhead"),
        P(SAMPLE, None, "kvhead"),
        P(SAMPLE, None, "kvhead"),
        P(SAMPLE, "kvhead", None),
        P(SAMPLE),
        P(SAMPLE_SPAN, "kvhead"),
        P(SAMPLE_SPAN, "kvhead"),
        P(SAMPLE, SPAN, "kvhead"),
        P(SAMPLE, SPAN, "kvhead"),
    )

    return jax.shard_map(
        shards,
        mesh=split,
        in_specs=placed,
        out_specs=(
            P(SAMPLE, SPAN, "kvhead"),
            P(SAMPLE_SPAN, "kvhead"),
            P(SAMPLE_SPAN, "kvhead"),
            P(SAMPLE, SPAN, "kvhead"),
            P(SAMPLE, SPAN, "kvhead"),
        ),
        check_vma=False,
    )
```

```python
import math

import jax
import jax.numpy as jnp
from jax import lax
from jax.experimental import pallas as pl
from jax.experimental.pallas import tpu as pltpu
from jax.sharding import Mesh
from jax.sharding import PartitionSpec as P

HEAD_WIDTH = 128
SAMPLE = ("sample_0", "sample_1")
SPAN = ("span_0", "span_1")
SAMPLE_SPAN = SAMPLE + SPAN
ALONG_X, ALONG_Y = "span_0", ("sample_1", "span_1")
GROUP = 7
CLASSES = 8
SLOTS = 24
LIVE = 144
STATS = GROUP * HEAD_WIDTH
INTERPRET = False
KEY_BLOCK, ROW_BLOCK = 512, 512
VMEM_BYTES = 24 * 1024 * 1024
BF16 = jnp.bfloat16
F32 = jnp.float32
SCALE = 1.0 / math.sqrt(HEAD_WIDTH)
EXACT = lax.Precision.HIGHEST


def exchange(tiles, axes):
    return lax.all_to_all(tiles, axes, split_axis=0, concat_axis=0, tiled=True)


def dot(a, b, ca, cb):
    return lax.dot_general(a, b, (((ca,), (cb,)), ((), ())), preferred_element_type=F32)


def call(body, out_shape, *args, small=True, **kw):
    params = pltpu.CompilerParams(vmem_limit_bytes=VMEM_BYTES if small else None)
    return pl.pallas_call(
        body, out_shape=out_shape, interpret=INTERPRET, compiler_params=params, **kw
    )(*args)


def stat_lanes(shape):
    lane = lax.broadcasted_iota(jnp.int32, shape, 1)
    group = jnp.zeros(shape, jnp.int32)
    for edge in range(GROUP, 6 * GROUP, GROUP):
        group = group + jnp.where(lane >= edge, 1, 0)
    piece = jnp.where(group >= 3, group - 3, group)
    return lane, lane - GROUP * group, piece


def pick_kernel(p_ref, turn_ref, live_ref, q_ref, o_ref, g_ref, norm_ref, out_ref):
    p, turn, live = p_ref[0], turn_ref[0], live_ref[0]
    row = lax.broadcasted_iota(jnp.int32, (64, 256), 0)
    i = lax.broadcasted_iota(jnp.int32, (64, 256), 1)
    hit = (i % 8 == p) & (i < live) & ((turn + i // 8) % 8 == row // 8) & (i // 64 == row % 4)
    pick_q = jnp.where(hit & (row % 8 < 4), 1.0, 0.0)
    pick_g = jnp.where(hit & (row % 8 >= 4), 1.0, 0.0).astype(BF16)
    lane, head_of, piece = stat_lanes((64, HEAD_WIDTH))
    pick_q_low = pick_q.astype(BF16)
    both = dot(pick_q_low, q_ref[...], 1, 0) + dot(pick_g, g_ref[...], 1, 0)
    out_ref[:, 0, :, 0:STATS] = both.reshape(8, 8, STATS).astype(BF16)
    product = dot(pick_q_low, o_ref[...], 1, 0) * dot(pick_q_low, g_ref[...], 1, 0)
    stat = jnp.zeros((64, HEAD_WIDTH), F32)
    for inner in range(GROUP):
        mine = head_of == inner
        part = product[:, inner * HEAD_WIDTH : (inner + 1) * HEAD_WIDTH]
        delta = jnp.sum(part, axis=1, keepdims=True)
        norm = norm_ref[inner]
        norm = jnp.sum(pick_q * norm, axis=1, keepdims=True) * math.sqrt(HEAD_WIDTH)
        stat = jnp.where(mine & (lane < 3 * GROUP), norm, stat)
        stat = jnp.where(mine & (lane >= 3 * GROUP) & (lane < 6 * GROUP), delta, stat)
    high = stat.astype(BF16).astype(F32)
    middle = (stat - high).astype(BF16).astype(F32)
    low = stat - high - middle
    stat = jnp.where(piece == 0, high, jnp.where(piece == 1, middle, low))
    stat = jnp.where(lane == 6 * GROUP, live.astype(F32), stat)
    out_ref[:, 0, :, STATS:] = stat.reshape(8, 8, HEAD_WIDTH).astype(BF16)


def compact_kernel(p_ref, z_ref, rows_ref, out_ref):
    rows = rows_ref[...].reshape(128, 1024)
    shape = (128, 128)
    row = lax.broadcasted_iota(jnp.int32, shape, 0)
    col = lax.broadcasted_iota(jnp.int32, shape, 1)
    length = rows[:, STATS + 6 * GROUP : STATS + 6 * GROUP + 1].astype(F32)
    length = jnp.broadcast_to(length, shape).astype(jnp.int32)
    count = (length - p_ref[0] + 7) >> 3
    valid = 8 * (row & 3) + ((z_ref[0] - (row >> 3)) & 7) < count
    earlier = jnp.where(((col >> 3) < (row >> 3)) & (((col >> 2) & 1) == 0), 1.0, 0.0)
    before = dot(earlier.astype(BF16), jnp.where(valid, 1.0, 0.0).astype(BF16), 1, 0)
    place = before.astype(jnp.int32) + (row & 3) + SLOTS * ((row >> 2) & 1)
    pick = jnp.where(valid & (place == col), 1.0, 0.0).astype(BF16)
    rows = dot(pick, rows, 0, 0)[0 : 2 * SLOTS].astype(BF16)
    for copy in range(out_ref.shape[0]):
        out_ref[copy] = rows


def prompt_kernel(in_slot_ref, out_slot_ref, rows_ref, *refs):
    kv_refs, kvg_refs = refs[0:4], refs[4:8]
    gq_ref, q_scr, g_scr, acc_ref, back_ref = refs[8:]
    acc_ref[...] = jnp.zeros_like(acc_ref)
    slot = in_slot_ref[0:1, :]
    hit = lax.broadcasted_iota(jnp.int32, (2 * LIVE, slot.shape[1]), 0) == slot
    pick = jnp.where(hit, 1.0, 0.0).astype(BF16)
    rows = dot(pick, rows_ref[...].reshape(slot.shape[1], -1), 1, 0).astype(BF16)
    lane, head_of, _ = stat_lanes((LIVE, HEAD_WIDTH))
    stats = rows[0:LIVE, STATS:]
    zero = jnp.zeros((), BF16)
    for head in range(GROUP):
        place = slice(head * LIVE, (head + 1) * LIVE)
        lanes = slice(head * HEAD_WIDTH, (head + 1) * HEAD_WIDTH)
        mine = head_of == head
        q_scr[place, 0:HEAD_WIDTH] = rows[0:LIVE, lanes]
        q_scr[place, HEAD_WIDTH:] = jnp.where(mine & (lane < 3 * GROUP), stats, zero)
        g_scr[place, 0:HEAD_WIDTH] = rows[LIVE:, lanes]
        g_scr[place, HEAD_WIDTH:] = jnp.where(
            mine & (lane >= 3 * GROUP) & (lane < 6 * GROUP), stats, zero
        )
    q_scr[GROUP * LIVE :, :] = jnp.zeros((1024 - GROUP * LIVE, 2 * HEAD_WIDTH), BF16)
    g_scr[GROUP * LIVE :, :] = jnp.zeros((1024 - GROUP * LIVE, 2 * HEAD_WIDTH), BF16)

    lane = lax.broadcasted_iota(jnp.int32, (KEY_BLOCK, HEAD_WIDTH), 1)
    minus = jnp.where(lane < 6 * GROUP, -1.0, 0.0).astype(BF16)
    for kv_ref, kvg_ref in zip(kv_refs, kvg_refs):
        for first in range(0, 1024, 2 * KEY_BLOCK):
            starts = range(first, first + 2 * KEY_BLOCK, 256)
            keys = jnp.concatenate([kv_ref[k : k + 128, :] for k in starts], axis=0)
            values = jnp.concatenate([kv_ref[k + 128 : k + 256, :] for k in starts], axis=0)
            turned = keys.T
            wide_keys = jnp.concatenate([keys, minus], axis=1)
            wide_values = jnp.concatenate([values, minus], axis=1)
            gk = jnp.zeros(keys.shape, F32)
            gv = jnp.zeros(keys.shape, F32)
            for part in range(0, 1024, ROW_BLOCK):
                rows = slice(part, part + ROW_BLOCK)
                prob = jnp.exp2(dot(wide_keys, q_scr[rows, :], 1, 1) * (SCALE / math.log(2)))
                sgrad = (prob * dot(wide_values, g_scr[rows, :], 1, 1)).astype(BF16)
                gv = gv + dot(prob.astype(BF16), g_scr[rows, 0:HEAD_WIDTH], 1, 0)
                gk = gk + dot(sgrad, q_scr[rows, 0:HEAD_WIDTH], 1, 0)
                acc_ref[:, rows] += dot(turned, sgrad, 1, 0)
            for n, k in enumerate(starts):
                kvg_ref[k : k + 128, :] = (gk[128 * n : 128 * n + 128] * SCALE).astype(BF16)
                kvg_ref[k + 128 : k + 256, :] = gv[128 * n : 128 * n + 128].astype(BF16)

    back_ref[...] = jnp.zeros_like(back_ref)
    sums = acc_ref[...].T
    for head in range(GROUP):
        lanes = slice(head % 4 * HEAD_WIDTH, (head % 4 + 1) * HEAD_WIDTH)
        part = (sums[head * LIVE : (head + 1) * LIVE, :] * SCALE).astype(BF16)
        back_ref[head // 4 * LIVE : (head // 4 + 1) * LIVE, lanes] = part
    slot = out_slot_ref[0:1, :]
    hit = lax.broadcasted_iota(jnp.int32, (2 * LIVE, slot.shape[1]), 0) == slot
    pick = jnp.where(hit, 1.0, 0.0).astype(BF16)
    gq_ref[...] = dot(pick, back_ref[...], 0, 0).reshape(gq_ref.shape).astype(BF16)


def prompt_terms(in_slot, out_slot, rows, *kv):
    *kv_grads, gq = call(
        prompt_kernel,
        [pltpu.HBM((1024, HEAD_WIDTH), BF16)] * 4 + [pltpu.HBM((128, 8, 512), BF16)],
        in_slot,
        out_slot,
        rows,
        *kv,
        out_specs=[pl.BlockSpec(memory_space=pltpu.VMEM)] * 5,
        scratch_shapes=[
            pltpu.VMEM((1024, 2 * HEAD_WIDTH), BF16),
            pltpu.VMEM((1024, 2 * HEAD_WIDTH), BF16),
            pltpu.VMEM((HEAD_WIDTH, 1024), F32),
            pltpu.VMEM((2 * LIVE, 512), BF16),
        ],
    )
    return kv_grads, gq


def final_kernel(parts_ref, own_ref, out_ref, sum_ref):
    for half in range(2):
        for p in range(CLASSES):
            total = parts_ref[half * 8 + p].astype(F32)
            for z in range(1, 8):
                total = total + parts_ref[z * 16 + half * 8 + p].astype(F32)
            for head in range(GROUP):
                rows = slice(head // 4 * 4, head // 4 * 4 + 4)
                part = total[rows, head % 4 * HEAD_WIDTH : (head % 4 + 1) * HEAD_WIDTH]
                first = (half * GROUP + head) * 32 + p
                sum_ref[pl.ds(first, 4, stride=8), :] = part
    for head in range(2 * GROUP):
        lanes = slice(head * HEAD_WIDTH, (head + 1) * HEAD_WIDTH)
        out_ref[:, lanes] = (sum_ref[head * 32 : head * 32 + 32, :] + own_ref[:, lanes]).astype(BF16)


def pack_kernel(info, pk_ref, pv_ref, sk_ref, sv_ref, own_ref, other_ref):
    half = info[0]
    low, high = slice(0, HEAD_WIDTH), slice(HEAD_WIDTH, 2 * HEAD_WIDTH)
    for k, ref in enumerate((pk_ref, pv_ref)):
        rows = slice(128 * k, 128 * k + 128)
        own_ref[rows, :] = jnp.where(half == 0, ref[:, low], ref[:, high])
        other_ref[rows, :] = jnp.where(half == 0, ref[:, high], ref[:, low])
    for k, (ref, lanes) in enumerate(((sk_ref, low), (sk_ref, high), (sv_ref, low), (sv_ref, high))):
        own_ref[256 + 32 * k : 288 + 32 * k, :] = ref[:, lanes]


def join_kernel(own_ref, beside_ref, third_ref, fourth_ref, out_ref):
    for k, ref in enumerate((own_ref, beside_ref, third_ref, fourth_ref)):
        out_ref[256 * k : 256 * k + 256, :] = ref[0:256, :]
    out_ref[1024:1152, :] = own_ref[256:384, :]
    out_ref[1152:1280, :] = beside_ref[256:384, :]


def relay_kernel(own_ref, relayed_ref, out_ref):
    out_ref[...] = (own_ref[...].astype(F32) + relayed_ref[...].astype(F32)).astype(BF16)


def x_sum_kernel(a_ref, b_ref, c_ref, *out_refs):
    for k, out_ref in enumerate(out_refs):
        rows = slice(256 * k, 256 * k + 256)
        total = a_ref[rows, :].astype(F32) + b_ref[rows, :].astype(F32)
        out_ref[...] = (total + c_ref[rows, :].astype(F32)).astype(BF16)


def y_sum_kernel(info, a_ref, b_ref, c_ref, d_ref, k_ref, v_ref):
    half = info[0]
    own = a_ref[...].astype(F32) + b_ref[...].astype(F32)
    other = c_ref[...].astype(F32) + d_ref[...].astype(F32)
    low = jnp.where(half == 0, own, other).astype(BF16)
    high = jnp.where(half == 0, other, own).astype(BF16)
    for k, ref in enumerate((k_ref, v_ref)):
        ref[:, 0:HEAD_WIDTH] = low[128 * k : 128 * k + 128]
        ref[:, HEAD_WIDTH:] = high[128 * k : 128 * k + 128]


def shifted(value, by):
    return lax.ppermute(value, ALONG_X, [(k, (k + by) % 4) for k in range(4)])


def crossed(value, by):
    return lax.ppermute(value, ALONG_Y, [(k, k ^ by) for k in range(4)])


def self_kernel(
    p_ref, live_ref, q_ref, o_ref, g_ref, norm_ref, kv0_ref, kv1_ref, kv2_ref, kv3_ref,
    gk_ref, gv_ref, gq_ref,
):
    p, live = p_ref[0], live_ref[0]
    rows_total = q_ref.shape[0]
    i_row = lax.broadcasted_iota(jnp.int32, (32, rows_total), 1)
    j_row = lax.broadcasted_iota(jnp.int32, (32, rows_total), 0) + p * 32
    live_row = lax.broadcasted_iota(jnp.int32, (rows_total, HEAD_WIDTH), 0) < live
    live_own = lax.broadcasted_iota(jnp.int32, (32, HEAD_WIDTH), 0) + p * 32 < live
    zero = jnp.zeros((), BF16)
    ones = jnp.ones((8, HEAD_WIDTH), F32)
    own = pl.ds(pl.multiple_of(p * 32, 32), 32)
    diagonal = i_row == j_row
    kv_refs = (kv0_ref, kv1_ref, kv2_ref, kv3_ref)
    lane = lax.broadcasted_iota(jnp.int32, (1, rows_total), 1)
    block = lane // 32
    from_span = (p // 2 + 4 - block // 2) % 4 * 2 + (p % 2 + block % 2) % 2
    position = from_span * 32 + lane % 32
    kv = pl.program_id(0)
    def piece(ref, which, kind):
        first = 1024 + 128 * which + 32 * (2 * kind + kv)
        return ref[pl.ds(pl.multiple_of(first, 32), 32), :]

    keys, values = piece(kv0_ref, 0, 0), piece(kv0_ref, 0, 1)
    all_keys = jnp.concatenate([piece(r, w, 0) for r in kv_refs for w in range(2)], axis=0)
    all_values = jnp.concatenate([piece(r, w, 1) for r in kv_refs for w in range(2)], axis=0)
    gk = jnp.zeros((32, HEAD_WIDTH), F32)
    gv = jnp.zeros((32, HEAD_WIDTH), F32)
    for inner in range(GROUP):
        head = inner
        lanes = slice(head * HEAD_WIDTH, (head + 1) * HEAD_WIDTH)
        q = q_ref[:, lanes]
        g = jnp.where(live_row, g_ref[:, lanes], zero)
        product = g.astype(F32) * o_ref[:, lanes].astype(F32)
        delta = lax.dot_general(
            ones, product, (((1,), (1,)), ((), ())), precision=EXACT, preferred_element_type=F32
        )
        prob = jnp.exp(dot(keys, q, 1, 1) * SCALE - norm_ref[head])
        prob = jnp.where(j_row <= i_row, prob, 0.0)
        sgrad = prob * (dot(values, g, 1, 1) - delta[0:1, :])
        gv = gv + dot(prob.astype(BF16), g, 1, 0)
        gk = gk + dot(sgrad.astype(BF16), q, 1, 0)
        q_own, g_own = q_ref[own, lanes], g_ref[own, lanes]
        g_own = jnp.where(live_own, g_own, zero)
        product = g_own.astype(F32) * o_ref[own, lanes].astype(F32)
        delta_own = jnp.sum(product, axis=1, keepdims=True)
        norm_own = jnp.sum(jnp.where(diagonal, norm_ref[head], 0.0), axis=1, keepdims=True)
        prob = jnp.exp(dot(q_own, all_keys, 1, 1) * SCALE - norm_own)
        i_own = lax.broadcasted_iota(jnp.int32, prob.shape, 0) + p * 32
        prob = jnp.where(position <= i_own, prob, 0.0)
        sgrad = prob * (dot(g_own, all_values, 1, 1) - delta_own)
        gq_ref[:, lanes] = dot(sgrad.astype(BF16), all_keys, 1, 0) * SCALE
    gk_ref[...] = (gk * SCALE).astype(BF16)
    gv_ref[...] = gv.astype(BF16)


def shards(
    queries,
    outputs,
    grad_out,
    log_norms,
    lengths,
    prompt_key_rows,
    prompt_value_rows,
    slice_key_rows,
    slice_value_rows,
):
    z = lax.axis_index("sample_0")
    half = lax.axis_index("sample_1")
    p = lax.axis_index(SPAN)
    sample = 2 * z + half
    spans = lax.axis_size(SPAN)
    slice_rows = queries.shape[1]
    heads = queries.shape[2] // HEAD_WIDTH
    class_rows = slice_rows // CLASSES
    q, o, g = queries[0], outputs[0], grad_out[0]
    norms = log_norms.transpose(1, 0, 2)
    smem, vmem = pl.BlockSpec(memory_space=pltpu.SMEM), pl.BlockSpec(memory_space=pltpu.VMEM)

    picked = call(
        pick_kernel,
        jax.ShapeDtypeStruct((8, 2, 8, 1024), BF16),
        p[None],
        (sample % 8)[None],
        lengths,
        q,
        o,
        g,
        norms,
        grid=(2,),
        in_specs=[smem] * 3
        + [pl.BlockSpec((slice_rows, STATS), lambda k: (0, k))] * 3
        + [pl.BlockSpec((GROUP, 1, slice_rows), lambda k: (k, 0, 0))],
        out_specs=pl.BlockSpec((8, 1, 8, 1024), lambda k: (0, k, 0, 0)),
        small=False,
    )
    arrived = exchange(picked.reshape(16, 8, 1024), SAMPLE)

    packed = lambda rows: jax.ShapeDtypeStruct((rows, HEAD_WIDTH), BF16)
    own, other = call(
        pack_kernel,
        [packed(384), packed(256)],
        half[None],
        prompt_key_rows,
        prompt_value_rows,
        slice_key_rows[0],
        slice_value_rows[0],
        in_specs=[smem] + [vmem] * 4,
    )
    around = [own, crossed(own, 1), crossed(other, 2), crossed(other, 3)]
    column = call(join_kernel, packed(1280), *around)
    kv = [column] + [shifted(column, k) for k in (1, 2, 3)]

    all_lengths = arrived[:, 0, STATS + 6 * GROUP].astype(jnp.int32)
    live_of = jnp.clip((all_lengths - p + CLASSES - 1) // CLASSES, 0, class_rows)
    every_sample = jnp.arange(16)
    first = (jnp.arange(8)[None, :] - every_sample[:, None]) % 8
    held = jnp.clip((live_of[:, None] - first + 7) // 8, 0, 4)
    earlier = (every_sample[None, :] < every_sample[:, None])[:, :, None]
    before = jnp.sum(jnp.where(earlier, held[None], 0), axis=1)
    total = jnp.sum(held, axis=0)
    base = jnp.sum(jnp.where(jnp.arange(8)[None, :] < jnp.arange(8)[:, None], total[None], 0), axis=1)
    compact = call(
        compact_kernel,
        jax.ShapeDtypeStruct((8, 2 * SLOTS, 1024), BF16),
        p[None],
        z[None],
        arrived,
        in_specs=[smem, smem, vmem],
    )
    rows = exchange(compact, "sample_0")
    step = jnp.arange(SLOTS)[None, :]
    in_slot = base[:, None] + step
    in_slot = in_slot[:, None, :] + LIVE * jnp.arange(2)[None, :, None]
    in_slot = jnp.where((step < total[:, None])[:, None, :], in_slot, -1).reshape(1, 16 * SLOTS)
    k = jnp.arange(class_rows)
    holder = (k[None, :] + every_sample[:, None]) % 8
    chosen = holder[:, :, None] == jnp.arange(8)[None, None, :]
    slot_of = jnp.sum(jnp.where(chosen, (base[None, :] + before)[:, None, :], 0), axis=2)
    slot_of = jnp.where(k[None, :] < live_of[:, None], slot_of + k[None, :] // 8, -LIVE * 2)
    out_slot = slot_of.reshape(16, spans, 1, 4) + LIVE * jnp.arange(2)[None, None, :, None]
    out_slot = out_slot.reshape(1, 1024)

    kv_grads, gq_parts = prompt_terms(in_slot, out_slot, rows, *kv)
    relayed = shifted(kv_grads[2], -1)
    ahead = shifted(kv_grads[3], 1)
    gq_parts = exchange(gq_parts, SAMPLE_SPAN)
    joined = call(relay_kernel, packed(1024), kv_grads[1], relayed)
    behind = shifted(joined, -1)
    own_rows = slice_rows // spans
    own_shape = jax.ShapeDtypeStruct((own_rows, 2 * HEAD_WIDTH), BF16)
    gk_self, gv_self, gq_self = call(
        self_kernel,
        [own_shape, own_shape, jax.ShapeDtypeStruct((own_rows, heads * HEAD_WIDTH), F32)],
        p[None],
        lengths,
        q,
        o,
        g,
        norms,
        *kv,
        grid=(2,),
        in_specs=[smem] * 2
        + [pl.BlockSpec((slice_rows, STATS), lambda k: (0, k))] * 3
        + [pl.BlockSpec((GROUP, 1, slice_rows), lambda k: (k, 0, 0))]
        + [pl.BlockSpec((1280, HEAD_WIDTH), lambda k: (0, 0))] * 4,
        out_specs=[pl.BlockSpec((own_rows, HEAD_WIDTH), lambda k: (0, k))] * 2
        + [pl.BlockSpec((own_rows, STATS), lambda k: (0, k))],
        small=False,
    )
    parts = call(x_sum_kernel, [packed(256)] * 4, kv_grads[0], ahead, behind)
    parts = [parts[0]] + [crossed(parts[k], k) for k in (1, 2, 3)]
    prompt_shape = jax.ShapeDtypeStruct(prompt_key_rows.shape, BF16)
    gk_prompt, gv_prompt = call(
        y_sum_kernel,
        [prompt_shape, prompt_shape],
        half[None],
        *parts,
        in_specs=[smem] + [vmem] * 4,
    )
    grad_query = call(
        final_kernel,
        jax.ShapeDtypeStruct((own_rows, heads * HEAD_WIDTH), BF16),
        gq_parts,
        gq_self,
        scratch_shapes=[pltpu.VMEM((heads * own_rows, HEAD_WIDTH), F32)],
    )
    return grad_query[None], gk_prompt, gv_prompt, gk_self[None], gv_self[None]


def solution(mesh):
    split = Mesh(
        mesh.devices.reshape(8, 2, 4, 2, mesh.shape["kvhead"]), SAMPLE_SPAN + ("kvhead",)
    )
    placed = (
        P(SAMPLE, None, "kvhead"),
        P(SAMPLE, None, "kvhead"),
        P(SAMPLE, None, "kvhead"),
        P(SAMPLE, "kvhead", None),
        P(SAMPLE),
        P(SAMPLE_SPAN, "kvhead"),
        P(SAMPLE_SPAN, "kvhead"),
        P(SAMPLE, SPAN, "kvhead"),
        P(SAMPLE, SPAN, "kvhead"),
    )

    return jax.shard_map(
        shards,
        mesh=split,
        in_specs=placed,
        out_specs=(
            P(SAMPLE, SPAN, "kvhead"),
            P(SAMPLE_SPAN, "kvhead"),
            P(SAMPLE_SPAN, "kvhead"),
            P(SAMPLE, SPAN, "kvhead"),
            P(SAMPLE, SPAN, "kvhead"),
        ),
        check_vma=False,
    )
```
